256 devices in a mesh: seq: 64 (over x, z, core), head: 4 (over y).
Axes of the slice: x: 4, y: 4, z: 8, core: 2. Of those that a mesh axis runs over, the one named last changes fastest.
Arguments:
- tokens: bfloat16 [2, 8192, 1024], P(None, 'seq', 'head'), may hold values from -6 to 6
- input_norm_gain: float32 [1024], replicated, may hold values from 0.1 to 1.9
- query_key_value_weight: bfloat16 [1024, 3, 1024], P(None, None, 'head'), may hold values from -0.1875 to 0.1875
- forget_gate_weight: bfloat16 [1024, 1024], P(None, 'head'), may hold values from -0.1875 to 0.1875
- convolution_filter_taps: float32 [2, 4, 3, 1024], P(None, None, None, 'head'), may hold values from -3 to 3
- slot_forget_rate: float32 [16, 64], P('head'), may hold values from 2.4414063e-06 to 0.04
- extra_forget_log: float32 [2, 8192], P(None, 'seq'), may hold values from 0 to 1.4, as said below
- head_norm_gain: float32 [16, 64], P('head'), may hold values from 0.1 to 1.9
- output_projection_weight: bfloat16 [1024, 1024], P('head'), may hold values from -0.1875 to 0.1875
- feedforward_norm_gain: float32 [1024], replicated, may hold values from 0.1 to 1.9
- up_projection_weight: bfloat16 [1024, 4096], P(None, 'head'), may hold values from -0.1875 to 0.1875
- down_projection_weight: bfloat16 [4096, 1024], P('head'), may hold values from -0.09375 to 0.09375
Outputs:
- layer_out: bfloat16 [2, 8192, 1024], P(None, 'seq', 'head')
The draws below stay inside these ranges and needn't reach their ends.
Inputs may be any that keep to these rules, and one draw needn't show every extreme that they name: `extra_forget_log`: one value per position of a sequence, zero at most positions.
All inputs are finite; a program needn't handle non-finite values.
Results may differ from the reference program's by a relative error of at most 0.01.
Values may be sent and summed in bfloat16 or wider, within the bound.
No kernel may reach another device: no remote copies, remote signals or barrier semaphores. Data moves between devices by JAX's collectives and lax.ppermute only.
A program may use at most 128 MiB of HBM per device.

```python
import jax
import jax.numpy as jnp
from jax import lax

D = 1024
HEADS = 16
HD = 64
SLOTS = 64
FF = 4096
SPAN = 64
BATCH = 2
SEQ_LEN = 8192


def draw_slot_forget_rate(key, part):
    first, second, third = jax.random.split(jax.random.fold_in(key, 11), 3)
    choose = jax.random.uniform(first, (HEADS, SLOTS), dtype=jnp.float32)
    share = 0.5
    slower = jnp.exp(jax.random.uniform(second, (HEADS, SLOTS), jnp.float32, jnp.log(0.02), jnp.log(0.4))) / SEQ_LEN
    faster = jnp.exp(jax.random.uniform(third, (HEADS, SLOTS), jnp.float32, jnp.log(0.02), jnp.log(0.04)))
    return jnp.where(choose < share, slower, faster).astype(jnp.float32)


def draw_extra_forget_log(key, part):
    first, second = jax.random.split(jax.random.fold_in(key, 23))
    places = jax.random.randint(first, (BATCH, 2), 0, SEQ_LEN)
    depth = jax.random.uniform(second, (BATCH, 2), jnp.float32, 0.22, 0.7)
    hitting = jnp.arange(SEQ_LEN)[None, None, :] == places[:, :, None]
    return jnp.sum(jnp.where(hitting, depth[:, :, None], 0.0), axis=1).astype(jnp.float32)


def steps_of(key, dims, cuts, least, largest):
    level, own = 1.0, jax.random.fold_in(key, 6)
    for position, shards_of in cuts:
        heights = jnp.exp(jax.random.uniform(jax.random.fold_in(own, position), (shards_of,), jnp.float32, least / len(cuts), largest / len(cuts)))
        level = level * jnp.repeat(heights, dims[position] // shards_of).reshape([-1 if axis == position else 1 for axis in range(len(dims))])
    return level


def gaussian(stream_key, extent, scale, bound, shards=(), kind=jnp.bfloat16):
    values = scale * jax.random.normal(stream_key, extent, jnp.float32)
    if shards:
        values = values * steps_of(stream_key, extent, shards, -0.22, 0.18)
    return jnp.clip(values, -bound, bound).astype(kind)


def setup_inputs(seed: int = 0) -> dict:
    keys = jax.random.split(jax.random.key(seed), 13)
    return {
        "tokens": gaussian(keys[0], (BATCH, SEQ_LEN, D), 1.0, 6.0, ((1, 64), (2, 4))),
        "input_norm_gain": jnp.clip(1.0 + 0.18 * jax.random.normal(keys[1], (D,), jnp.float32), 0.1, 1.9),
        "query_key_value_weight": gaussian(keys[2], (D, 3, HEADS * HD), D ** -0.5, 0.1875, ((2, 4),)),
        "forget_gate_weight": gaussian(keys[3], (D, HEADS * SLOTS), D ** -0.5, 0.1875, ((1, 4),)),
        "convolution_filter_taps": gaussian(keys[4], (2, 4, 3, HEADS * HD), 0.6, 3.0, ((3, 4),), jnp.float32),
        "slot_forget_rate": draw_slot_forget_rate(jax.random.fold_in(keys[12], 71), 0),
        "extra_forget_log": draw_extra_forget_log(jax.random.fold_in(keys[12], 71), 0),
        "head_norm_gain": jnp.clip(1.0 + 0.18 * jax.random.normal(keys[7], (HEADS, HD), jnp.float32), 0.1, 1.9),
        "output_projection_weight": gaussian(keys[8], (HEADS * HD, D), (HEADS * HD) ** -0.5, 0.1875, ((0, 4),)),
        "feedforward_norm_gain": jnp.clip(1.0 + 0.18 * jax.random.normal(keys[9], (D,), jnp.float32), 0.1, 1.9),
        "up_projection_weight": gaussian(keys[10], (D, FF), D ** -0.5, 0.1875, ((1, 4),)),
        "down_projection_weight": gaussian(keys[11], (FF, D), FF ** -0.5, 0.09375, ((0, 4),)),
    }


EPSILON = 1e-06
HIGHEST = lax.Precision.HIGHEST

def normalize(values, gain):
    return values * lax.rsqrt(lax.optimization_barrier(jnp.mean(values * values, axis=-1, keepdims=True)) + EPSILON) * gain

def convolve(padded, taps, backward):
    length = padded.shape[1] - 6
    running = jnp.zeros((padded.shape[0], length, padded.shape[2]), jnp.float32)
    for offset in range(4):
        first_row = 3 + offset if backward else 3 - offset
        running = running + taps[offset] * padded[:, first_row:first_row + length]
    return jax.nn.silu(running).astype(jnp.bfloat16)

def split_heads(mixed, head_count, head_size):
    grouped = mixed.astype(jnp.float32).reshape(mixed.shape[0], mixed.shape[1], 3, head_count, head_size)
    grouped = jnp.transpose(grouped, (2, 0, 3, 1, 4))
    return (grouped[0], grouped[1], grouped[2])

def log_decay_values(gate_scores, slot_forget_rate, extra_forget_log):
    head_count, slot_count = slot_forget_rate.shape
    gate_opening = jax.nn.sigmoid(gate_scores.reshape(gate_scores.shape[0], gate_scores.shape[1], head_count, slot_count))
    log_decay_total = -2.0 * slot_forget_rate * gate_opening - extra_forget_log[:, :, None, None]
    return jnp.transpose(log_decay_total, (0, 2, 1, 3))

def flipped(array):
    return jnp.flip(array, axis=2)

def span_pass(state, block):
    queries, keys_in, values, log_decay_total = block
    state_key, state_value = state
    cumulative = jnp.cumsum(log_decay_total, axis=2)
    inflow = -jnp.expm1(log_decay_total)
    growth = jnp.exp(cumulative)
    shrink = jnp.exp(-cumulative) * inflow
    length = log_decay_total.shape[2]
    causal = (jnp.arange(length)[:, None] >= jnp.arange(length)[None, :]).astype(jnp.float32)
    intersection = jnp.einsum('bhtd,bhjd->bhtj', queries, keys_in, precision=HIGHEST) * causal
    scores = jnp.einsum('bhtj,bhjs->bhts', intersection, shrink, precision=HIGHEST)
    scores = growth * (scores + jnp.einsum('bhsd,bhtd->bhts', state_key, queries, precision=HIGHEST))
    attend = jax.nn.softmax(scores, axis=-1)
    weighted = attend * growth
    mixing = jnp.einsum('bhts,bhjs->bhtj', weighted, shrink, precision=HIGHEST) * causal
    output = jnp.einsum('bhtj,bhjd->bhtd', mixing, values, precision=HIGHEST)
    output = output + jnp.einsum('bhts,bhsd->bhtd', weighted, state_value, precision=HIGHEST)
    ending = jnp.exp(cumulative[:, :, -1, :])
    remain = ending[:, :, None, :] * shrink
    state_key = ending[..., None] * state_key + jnp.einsum('bhjs,bhjd->bhsd', remain, keys_in, precision=HIGHEST)
    state_value = ending[..., None] * state_value + jnp.einsum('bhjs,bhjd->bhsd', remain, values, precision=HIGHEST)
    return ((state_key, state_value), output)

def recurrence(queries, keys_in, values, log_decay_total, state):
    batch_size, head_count, length = (queries.shape[0], queries.shape[1], queries.shape[2])
    blocks = length // SPAN

    def arrange(array):
        shaped = array.reshape(batch_size, head_count, blocks, SPAN, array.shape[3])
        return jnp.moveaxis(shaped, 2, 0)
    ignored, output = lax.scan(span_pass, state, (arrange(queries), arrange(keys_in), arrange(values), arrange(log_decay_total)))
    return jnp.moveaxis(output, 0, 2).reshape(batch_size, head_count, length, output.shape[-1])

def reference(tokens, input_norm_gain, query_key_value_weight, forget_gate_weight, convolution_filter_taps, slot_forget_rate, extra_forget_log, head_norm_gain, output_projection_weight, feedforward_norm_gain, up_projection_weight, down_projection_weight):
    batch_size, length, width = tokens.shape
    head_count, slot_count = slot_forget_rate.shape
    head_size = head_norm_gain.shape[1]
    normed = normalize(tokens.astype(jnp.float32), input_norm_gain).astype(jnp.bfloat16)
    projected = jnp.dot(normed, query_key_value_weight.reshape(width, 3 * head_count * head_size), preferred_element_type=jnp.float32).astype(jnp.bfloat16)
    padded = jnp.pad(projected.astype(jnp.float32), ((0, 0), (3, 3), (0, 0)))
    taps = convolution_filter_taps.reshape(2, 4, 3 * head_count * head_size)
    gate_scores = jnp.dot(normed, forget_gate_weight, preferred_element_type=jnp.float32)
    log_decay_total = log_decay_values(gate_scores, slot_forget_rate, extra_forget_log)
    zero_state = (jnp.zeros((batch_size, head_count, slot_count, head_size), jnp.float32), jnp.zeros((batch_size, head_count, slot_count, head_size), jnp.float32))
    forward_parts = split_heads(convolve(padded, taps[0], False), head_count, head_size)
    forward_out = recurrence(forward_parts[0], forward_parts[1], forward_parts[2], log_decay_total, zero_state)
    reverse_parts = [flipped(member) for member in split_heads(convolve(padded, taps[1], True), head_count, head_size)]
    reverse_out = flipped(recurrence(reverse_parts[0], reverse_parts[1], reverse_parts[2], flipped(log_decay_total), zero_state))
    gain_shape = head_norm_gain[None, :, None, :]
    combined = normalize(forward_out, gain_shape) + normalize(reverse_out, gain_shape)
    attention = jnp.transpose(combined, (0, 2, 1, 3)).reshape(batch_size, length, head_count * head_size).astype(jnp.bfloat16)
    residual = (tokens.astype(jnp.float32) + jnp.dot(attention, output_projection_weight, preferred_element_type=jnp.float32)).astype(jnp.bfloat16)
    mlp_in = normalize(residual.astype(jnp.float32), feedforward_norm_gain).astype(jnp.bfloat16)
    hidden = jax.nn.gelu(jnp.dot(mlp_in, up_projection_weight, preferred_element_type=jnp.float32)).astype(jnp.bfloat16)
    return (residual.astype(jnp.float32) + jnp.dot(hidden, down_projection_weight, preferred_element_type=jnp.float32)).astype(jnp.bfloat16)
```

```python
import jax
import jax.numpy as jnp
from jax import lax
from jax.experimental import pallas as pl
from jax.experimental.pallas import tpu as pltpu
from jax.sharding import Mesh
from jax.sharding import PartitionSpec as P

CHIPS = ("x", "z")
SEQ = ("x", "z", "core")
EPSILON = 1e-06
BF16 = jnp.bfloat16
F32 = jnp.float32
HIGHEST = lax.Precision.HIGHEST
SPAN = 64
ROWS = 256
LANES = 256
SPANS = ROWS // SPAN


def nn(a, b, precision=None):
    return lax.dot_general(
        a, b, (((1,), (0,)), ((), ())), preferred_element_type=F32, precision=precision
    )


def nt(a, b):
    return lax.dot_general(a, b, (((1,), (1,)), ((), ())), preferred_element_type=F32)


def tn(a, b, precision=None):
    return lax.dot_general(
        a, b, (((0,), (0,)), ((), ())), preferred_element_type=F32, precision=precision
    )


def iota(shape, dim):
    return lax.broadcasted_iota(jnp.int32, shape, dim)


def in_first_head(rows):
    return iota((rows, 128), 1) < 64


def compact(blocks):
    first = in_first_head(64)
    left = jnp.where(first, blocks[0:64, 0:128], blocks[64:128, 0:128])
    right = jnp.where(first, blocks[128:192, 128:256], blocks[192:256, 128:256])
    return jnp.concatenate([left, right], axis=1)


def compact_rows(column):
    first = in_first_head(64)
    left = jnp.where(first, column[0:64], column[64:128])
    right = jnp.where(first, column[128:192], column[192:256])
    return jnp.concatenate([left, right], axis=1)


def minus_expm1(x):
    series = 1.0 + x * (1.0 / 7.0)
    for k in (6, 5, 4, 3, 2):
        series = 1.0 + x * (1.0 / k) * series
    return jnp.where(x > -0.3, -x * series, 1.0 - jnp.exp(x))


def as_column(row):
    picked = jnp.where(iota((128, 128), 0) == iota((128, 128), 1), row, 0.0)
    return jnp.sum(picked, axis=1, keepdims=True)


def split_kernel(tokens, extra, swap_out, a_out, b_out, mine_out):
    core = lax.axis_index("core")
    mine = tokens[core]
    other = tokens[1 - core]
    mine_out[...] = mine
    row = extra[pl.ds(1 - core, 1), :]
    high = row.astype(BF16).astype(F32)
    middle = (row - high).astype(BF16).astype(F32)
    low = row - high - middle
    line = iota((8, 256), 0)
    first = jnp.concatenate([high, middle], axis=1)
    second = jnp.concatenate([low, low], axis=1)
    packed = jnp.where(line == 0, first, jnp.where(line == 1, second, 0.0))
    swap_out[...] = jnp.concatenate([other.astype(F32), packed], axis=0).astype(BF16)
    wide_other = other.astype(F32)
    wide_mine = mine.astype(F32)
    a_out[...] = jnp.where(core == 1, wide_other[120:128], wide_other[0:8]).astype(BF16)
    b_out[...] = jnp.where(core == 1, wide_mine[120:128], wide_mine[0:8]).astype(BF16)


def front_kernel(
    part0, part1, part2, part3, gain, qkv_weight, gate_weight, taps, rate, extra, extra_other,
    qkv_out, cum_out, shrink_out, start_out, reach_out, sent_out, tokens_out,
    padded, decay,
):
    core = lax.axis_index("core")
    head = lax.axis_index("head")
    parts = (part0, part1, part2, part3)
    sources = [lax.rem(head + 4 - k, 4) for k in range(4)]
    own_rows = pl.multiple_of(core * 128, 128)
    other_rows = pl.multiple_of((1 - core) * 128, 128)
    square = jnp.zeros((ROWS + 16, 1), F32)
    for k in range(4):
        values = parts[k][...]
        tokens_out[sources[k], pl.ds(own_rows, 128), :] = values[0:128]
        tokens_out[sources[k], pl.ds(other_rows, 128), :] = values[128:256]
        wide = values.astype(F32)
        square = square + jnp.sum(wide * wide, axis=1, keepdims=True)
    scale = lax.rsqrt(square * (1.0 / 1024.0) + EPSILON)
    normed = [
        (parts[k][...].astype(F32) * scale * gain[pl.ds(sources[k], 1), :]).astype(BF16)
        for k in range(4)
    ]
    starts = [pl.multiple_of(source * 256, 256) for source in sources]
    own_pad = pl.multiple_of(8 + core * 128, 8)
    other_pad = pl.multiple_of(8 + (1 - core) * 128, 8)
    a_pad = pl.multiple_of(core * 264, 8)
    b_pad = pl.multiple_of((1 - core) * 264, 8)
    for i in range(3):
        total = nn(normed[0], qkv_weight[i, pl.ds(starts[0], 256), :])
        for k in range(1, 4):
            total = total + nn(normed[k], qkv_weight[i, pl.ds(starts[k], 256), :])
        total = total.astype(BF16).astype(F32)
        columns = slice(i * 256, (i + 1) * 256)
        padded[pl.ds(own_pad, 128), columns] = total[0:128]
        padded[pl.ds(other_pad, 128), columns] = total[128:256]
        padded[pl.ds(a_pad, 8), columns] = total[256:264]
        padded[pl.ds(b_pad, 8), columns] = total[264:272]
    gate = nn(normed[0], gate_weight[pl.ds(starts[0], 256), :])
    for k in range(1, 4):
        gate = gate + nn(normed[k], gate_weight[pl.ds(starts[k], 256), :])
    own_extra = as_column(extra[pl.ds(core, 1), :])
    sent = extra_other[...].astype(F32)
    other_extra = as_column(sent[0:1, 0:128] + sent[0:1, 128:256] + sent[1:2, 0:128])
    decays = -2.0 * rate[...] * jax.nn.sigmoid(gate[0:256])
    decay[pl.ds(own_rows, 128), :] = decays[0:128] - own_extra
    decay[pl.ds(other_rows, 128), :] = decays[128:256] - other_extra

    for i in range(3):
        columns = slice(i * 256, (i + 1) * 256)
        for direction in range(2):
            running = taps[direction, i, 0:1, :] * padded[8 : 8 + ROWS, columns]
            for j in range(1, 4):
                first = 8 + j if direction else 8 - j
                running = running + taps[direction, i, j : j + 1, :] * padded[
                    first : first + ROWS, columns
                ]
            qkv_out[direction, i] = (running * jax.nn.sigmoid(running)).astype(BF16)

    log_decay = decay[...]
    inflow = minus_expm1(log_decay)
    row, col = iota((ROWS, ROWS), 0), iota((ROWS, ROWS), 1)
    same = (row // SPAN) == (col // SPAN)
    earlier = (same & (col <= row)).astype(F32)
    later = (same & (col >= row)).astype(F32)
    spans = (iota((ROWS, 128 * SPANS), 0) // SPAN == iota((ROWS, 128 * SPANS), 1) // 128).astype(F32)
    span_totals = tn(log_decay, spans, HIGHEST)
    totals = [compact_rows(span_totals[:, n * 128 : (n + 1) * 128]) for n in range(SPANS)]
    factors = [jnp.exp(total) for total in totals]
    ends = []
    for direction in range(2):
        cumulative = nn(later if direction else earlier, log_decay, HIGHEST)
        cum_out[direction] = cumulative
        shrink_out[direction] = (jnp.exp(-cumulative) * inflow).astype(BF16)
        states = [jnp.zeros((SPAN, LANES), F32), jnp.zeros((SPAN, LANES), F32)]
        passed = jnp.zeros((SPAN, LANES), F32)
        for n in reversed(range(SPANS)) if direction else range(SPANS):
            rows = slice(n * SPAN, (n + 1) * SPAN)
            start_out[direction, n, 0] = states[0]
            start_out[direction, n, 1] = states[1]
            reach_out[direction, n] = jnp.exp(passed)
            local = cumulative[rows]
            last = local[0:1] if direction else local[SPAN - 1 : SPAN]
            remain = (jnp.exp(last - local) * inflow[rows]).astype(BF16)
            for which in range(2):
                added = compact(tn(remain, qkv_out[direction, 1 + which, rows, :]))
                states[which] = factors[n] * states[which] + added
            passed = passed + totals[n]
        ends.append(states)
    factor = jnp.exp(totals[0] + totals[1] + totals[2] + totals[3])
    high = factor.astype(BF16).astype(F32)
    lane = iota((SPAN, LANES), 1)
    factor_parts = jnp.where(lane % 64 < 32, high, factor - high)
    for which in range(2):
        for half in range(2):
            lanes = slice(half * 128, (half + 1) * 128)
            for block in range(8):
                rows = slice(block * 8, block * 8 + 8)
                sent_out[which * 16 + half * 8 + block] = jnp.concatenate(
                    [
                        ends[0][which][rows, lanes],
                        ends[1][which][rows, lanes],
                        factor_parts[rows, lanes],
                    ],
                    axis=0,
                ).astype(BF16)


def scan_kernel(pieces, states_out, wide):
    count = pieces.shape[0]
    first = iota((8, 128), 1) % 64 < 32
    factors, forward, backward = [], [], []
    for i in range(count):
        piece = pieces[i].astype(F32)
        both = piece[16:24]
        factors.append(both + jnp.where(first, pltpu.roll(both, 96, 1), pltpu.roll(both, 32, 1)))
        forward.append(piece[0:8])
        backward.append(piece[8:16])
    state = jnp.zeros((8, 128), F32)
    for i in range(count):
        wide[i, 0:8, :] = state
        state = factors[i] * state + forward[i]
    state = jnp.zeros((8, 128), F32)
    for i in reversed(range(count)):
        wide[i, 8:16, :] = state
        state = factors[i] * state + backward[i]
    states_out[...] = wide[...].astype(BF16)


def head_max(values):
    first = in_first_head(SPAN)
    halves = []
    for half in range(2):
        part = values[:, half * 128 : (half + 1) * 128]
        left = jnp.max(jnp.where(first, part, -jnp.inf), axis=1, keepdims=True)
        right = jnp.max(jnp.where(first, -jnp.inf, part), axis=1, keepdims=True)
        halves.append(jnp.where(first, left, right))
    return jnp.concatenate(halves, axis=1)


def attention_kernel(qkv, cumulative, shrink, start, reach, arrived, gain, out, entering):
    for m in range(32):
        which, half, block = m // 16, (m // 8) % 2, m % 8
        piece = arrived[m].astype(F32)
        for direction in range(2):
            entering[direction, which, block * 8 : block * 8 + 8, half * 128 : half * 128 + 128] = (
                piece[direction * 8 : direction * 8 + 8]
            )
    own = (iota((LANES, LANES), 0) // 64 == iota((LANES, LANES), 1) // 64).astype(BF16)
    position, other = iota((SPAN, LANES), 0), iota((SPAN, LANES), 1) % SPAN

    def expand(values):
        return jnp.concatenate([values] * 4, axis=0) * own

    for n in range(SPANS):
        rows = slice(n * SPAN, (n + 1) * SPAN)
        combined = jnp.zeros((SPAN, LANES), F32)
        for direction in range(2):
            seen = other >= position if direction else other <= position
            queries = qkv[direction, 0, rows, :]
            keys = expand(qkv[direction, 1, rows, :])
            values = expand(qkv[direction, 2, rows, :])
            lessen = expand(shrink[direction, rows, :])
            growth = jnp.exp(cumulative[direction, rows, :])
            reached = reach[direction, n]
            key_state = expand(
                (start[direction, n, 0] + reached * entering[direction, 0]).astype(BF16)
            )
            value_state = expand(
                (start[direction, n, 1] + reached * entering[direction, 1]).astype(BF16)
            )
            meeting = jnp.where(seen, nt(queries, keys), 0.0).astype(BF16)
            scores = growth * (nn(meeting, lessen) + nt(queries, key_state))
            powers = jnp.exp(scores - head_max(scores))
            attend = powers / nn(powers.astype(BF16), own)
            weighted = (attend * growth).astype(BF16)
            mixing = jnp.where(seen, nt(weighted, lessen), 0.0).astype(BF16)
            result = nn(mixing, values) + nn(weighted, value_state)
            mean = nn((result * result).astype(BF16), own) * (1.0 / 64.0)
            combined = combined + result * lax.rsqrt(mean + EPSILON) * gain[...]
        out[rows, :] = combined.astype(BF16)


def tail_kernel(
    part0, part1, part2, part3, weight0, weight1, weight2, weight3, tokens, gain, up, down,
    base_out, out1, out2, out3, residual, update,
):
    head = lax.axis_index("head")
    parts = (part0, part1, part2, part3)
    weights = (weight0, weight1, weight2, weight3)
    square = jnp.zeros((ROWS, 1), F32)
    for j in range(4):
        columns = slice(j * 256, (j + 1) * 256)
        total = nn(parts[0][...], weights[0][:, columns])
        for k in range(1, 4):
            total = total + nn(parts[k][...], weights[k][:, columns])
        value = (tokens[j].astype(F32) + total).astype(BF16).astype(F32)
        residual[j] = value
        square = square + jnp.sum(value * value, axis=1, keepdims=True)
    scale = lax.rsqrt(square * (1.0 / 1024.0) + EPSILON)
    entering = jnp.concatenate(
        [(residual[j] * scale * gain[j : j + 1, :]).astype(BF16) for j in range(4)], axis=1
    )
    hidden = jnp.concatenate(
        [
            jax.nn.gelu(nn(entering, up[:, j * 256 : (j + 1) * 256])).astype(BF16)
            for j in range(4)
        ],
        axis=1,
    )
    for j in range(4):
        update[j] = nn(hidden, down[:, j * 256 : (j + 1) * 256])
    base_out[...] = residual[head] + update[head]
    for k, out in ((1, out1), (2, out2), (3, out3)):
        out[...] = update[lax.rem(head + k, 4)].astype(BF16)


def finish_kernel(base, part1, part2, part3, kept_out, sent_out):
    core = lax.axis_index("core")

    def rows_of(which):
        rows = pl.ds(pl.multiple_of(which * 128, 128), 128)
        total = base[rows, :]
        for part in (part1, part2, part3):
            total = total + part[rows, :].astype(F32)
        return total.astype(BF16)

    kept_out[...] = rows_of(core)
    sent_out[...] = rows_of(1 - core)


def kernel(body, outs, scratch=(), flops=0):
    shapes = [jax.ShapeDtypeStruct(shape, dtype) for shape, dtype in outs]
    return pl.pallas_call(
        body,
        out_shape=shapes,
        scratch_shapes=[pltpu.VMEM(shape, dtype) for shape, dtype in scratch],
        compiler_params=pltpu.CompilerParams(vmem_limit_bytes=48 * 1024 * 1024),
        cost_estimate=pl.CostEstimate(flops=flops, bytes_accessed=1 << 20, transcendentals=0),
    )


def shifted(value, k):
    count = lax.axis_size("head")
    return lax.ppermute(value, "head", [(j, (j + k) % count) for j in range(count)])


def local(
    tokens,
    input_norm_gain,
    query_key_value_weight,
    forget_gate_weight,
    convolution_filter_taps,
    slot_forget_rate,
    extra_forget_log,
    head_norm_gain,
    output_projection_weight,
    feedforward_norm_gain,
    up_projection_weight,
    down_projection_weight,
):
    chips = lax.axis_size(CHIPS)
    swap_pairs = [(0, 1), (1, 0)]
    swap, edge_a, edge_b, mine = kernel(
        split_kernel,
        [((136, 256), BF16), ((8, 256), BF16), ((8, 256), BF16), ((128, 256), BF16)],
    )(tokens, extra_forget_log)
    ahead = [(2 * i - 1, 2 * i) for i in range(1, chips)]
    behind = [(2 * i + 2, 2 * i + 1) for i in range(chips - 1)]
    other = lax.ppermute(swap, "core", swap_pairs)
    halo_a = lax.ppermute(edge_a, SEQ, ahead + behind)
    halo_b = lax.ppermute(
        edge_b,
        SEQ,
        [(2 * i - 1, 2 * i + 1) for i in range(1, chips)]
        + [(2 * i + 2, 2 * i) for i in range(chips - 1)],
    )
    rows = jnp.concatenate([mine, other[:128], halo_a, halo_b], axis=0)
    parts = [rows] + [shifted(rows, k) for k in (1, 2, 3)]
    qkv, cumulative, shrink, start, reach, pieces, whole_tokens = kernel(
        front_kernel,
        [
            ((2, 3, ROWS, LANES), BF16),
            ((2, ROWS, LANES), F32),
            ((2, ROWS, LANES), BF16),
            ((2, SPANS, 2, SPAN, LANES), F32),
            ((2, SPANS, SPAN, LANES), F32),
            ((32, 24, 128), BF16),
            ((4, ROWS, 256), BF16),
        ],
        [((ROWS + 16, 768), F32), ((ROWS, LANES), F32)],
        10**9,
    )(
        *parts,
        input_norm_gain.reshape(4, 256),
        jnp.transpose(query_key_value_weight, (1, 0, 2)),
        forget_gate_weight,
        jnp.transpose(convolution_filter_taps, (0, 2, 1, 3)),
        slot_forget_rate.reshape(1, LANES),
        extra_forget_log,
        other[128:],
    )
    pieces, out_weight = lax.optimization_barrier((pieces, output_projection_weight))
    out_weights = [out_weight] + [shifted(out_weight, k) for k in (1, 2, 3)]
    held = lax.all_to_all(pieces, CHIPS, split_axis=0, concat_axis=0, tiled=True)
    (prefixes,) = kernel(
        scan_kernel, [((chips, 16, 128), BF16)], [((chips, 16, 128), F32)]
    )(held)
    arrived = lax.all_to_all(prefixes, CHIPS, split_axis=0, concat_axis=0, tiled=True)
    (attention,) = kernel(
        attention_kernel,
        [((ROWS, LANES), BF16)],
        [((2, 2, SPAN, LANES), F32)],
        10**9,
    )(
        qkv, cumulative, shrink, start, reach, arrived, head_norm_gain.reshape(1, LANES)
    )
    attended = [attention] + [shifted(attention, k) for k in (1, 2, 3)]
    base, out1, out2, out3 = kernel(
        tail_kernel,
        [((ROWS, 256), F32)] + [((ROWS, 256), BF16)] * 3,
        [((4, ROWS, 256), F32), ((4, ROWS, 256), F32)],
        2 * 10**9,
    )(
        *attended,
        *out_weights,
        whole_tokens,
        feedforward_norm_gain.reshape(4, 256),
        up_projection_weight,
        down_projection_weight,
    )
    kept, sent = kernel(
        finish_kernel, [((128, 256), BF16), ((128, 256), BF16)]
    )(base, shifted(out1, 1), shifted(out2, 2), shifted(out3, 3))
    returned = lax.ppermute(sent, "core", swap_pairs)
    first = lax.axis_index("core") == 0
    return jnp.stack([jnp.where(first, kept, returned), jnp.where(first, returned, kept)])


def solution(mesh):
    split = Mesh(
        mesh.devices.reshape(4, 8, 2, mesh.shape["head"]), ("x", "z", "core", "head")
    )
    placed = (
        P(None, SEQ, "head"),
        P(),
        P(None, None, "head"),
        P(None, "head"),
        P(None, None, None, "head"),
        P("head", None),
        P(None, SEQ),
        P("head", None),
        P("head", None),
        P(),
        P(None, "head"),
        P("head", None),
    )
    return jax.shard_map(
        local, mesh=split, in_specs=placed, out_specs=P(None, SEQ, "head"), check_vma=False
    )
```

```python
import jax
import jax.numpy as jnp
from jax import lax
from jax.experimental import pallas as pl
from jax.experimental.pallas import tpu as pltpu
from jax.sharding import Mesh
from jax.sharding import PartitionSpec as P

CHIPS = ("x", "z")
SEQ = ("x", "z", "core")
EPSILON = 1e-06
BF16 = jnp.bfloat16
F32 = jnp.float32
HIGHEST = lax.Precision.HIGHEST
SPAN = 64
ROWS = 256
LANES = 256
SPANS = ROWS // SPAN


def nn(a, b, precision=None):
    return lax.dot_general(
        a, b, (((1,), (0,)), ((), ())), preferred_element_type=F32, precision=precision
    )


def nt(a, b):
    return lax.dot_general(a, b, (((1,), (1,)), ((), ())), preferred_element_type=F32)


def tn(a, b, precision=None):
    return lax.dot_general(
        a, b, (((0,), (0,)), ((), ())), preferred_element_type=F32, precision=precision
    )


def iota(shape, dim):
    return lax.broadcasted_iota(jnp.int32, shape, dim)


def in_first_head(rows):
    return iota((rows, 128), 1) < 64


def compact(blocks):
    first = in_first_head(64)
    left = jnp.where(first, blocks[0:64, 0:128], blocks[64:128, 0:128])
    right = jnp.where(first, blocks[128:192, 128:256], blocks[192:256, 128:256])
    return jnp.concatenate([left, right], axis=1)


def compact_rows(column):
    first = in_first_head(64)
    left = jnp.where(first, column[0:64], column[64:128])
    right = jnp.where(first, column[128:192], column[192:256])
    return jnp.concatenate([left, right], axis=1)


def minus_expm1(x):
    series = 1.0 + x * (1.0 / 7.0)
    for k in (6, 5, 4, 3, 2):
        series = 1.0 + x * (1.0 / k) * series
    return jnp.where(x > -0.3, -x * series, 1.0 - jnp.exp(x))


def as_column(row):
    picked = jnp.where(iota((128, 128), 0) == iota((128, 128), 1), row, 0.0)
    return jnp.sum(picked, axis=1, keepdims=True)


def begin(pairs, semaphores):
    copies = [
        pltpu.make_async_copy(source, target, semaphores.at[k])
        for k, (source, target) in enumerate(pairs)
    ]
    for copy in copies:
        copy.start()
    return copies


def finish(copies):
    for copy in copies:
        copy.wait()


def in_lanes(heads):
    return jnp.concatenate([heads[h : h + 1, :] for h in range(4)], axis=1)


def gain_of(gain, source):
    return jnp.concatenate(
        [gain[pl.ds(2 * source, 1), :], gain[pl.ds(2 * source + 1, 1), :]], axis=1
    )


def warm_kernel(qkv_weight, gate_weight, qkv_out, gate_out, semaphores):
    finish(begin([(qkv_weight, qkv_out), (gate_weight, gate_out)], semaphores))


def split_kernel(
    tokens_in, extra_in, swap_out, a_out, b_out, mine_out, tokens, extra, semaphores
):
    core = lax.axis_index("core")
    finish(begin([(tokens_in, tokens), (extra_in, extra)], semaphores))
    mine = tokens[core]
    other = tokens[1 - core]
    mine_out[...] = mine
    row = extra[pl.ds(1 - core, 1), :]
    high = row.astype(BF16).astype(F32)
    middle = (row - high).astype(BF16).astype(F32)
    low = row - high - middle
    line = iota((8, 256), 0)
    first = jnp.concatenate([high, middle], axis=1)
    second = jnp.concatenate([low, low], axis=1)
    packed = jnp.where(line == 0, first, jnp.where(line == 1, second, 0.0))
    swap_out[...] = jnp.concatenate([other.astype(F32), packed], axis=0).astype(BF16)
    wide_other = other.astype(F32)
    wide_mine = mine.astype(F32)
    a_out[...] = jnp.where(core == 1, wide_other[120:128], wide_other[0:8]).astype(BF16)
    b_out[...] = jnp.where(core == 1, wide_mine[120:128], wide_mine[0:8]).astype(BF16)


def front_kernel(
    part0, part1, part2, part3, gain, qkv_weight, gate_weight, taps, rate, extra, extra_other,
    sent_out, query_out, kv_out, cum_out, shrink_out, start_out, reach_out, tokens_out,
    padded, decay, query, kv, cum, shrink, start, reach, tokens, semaphores,
):
    core = lax.axis_index("core")
    head = lax.axis_index("head")
    parts = (part0, part1, part2, part3)
    sources = [lax.rem(head + 4 - k, 4) for k in range(4)]
    own_rows = pl.multiple_of(core * 128, 128)
    other_rows = pl.multiple_of((1 - core) * 128, 128)
    square = jnp.zeros((ROWS + 16, 1), F32)
    for k in range(4):
        values = parts[k][...]
        tokens[sources[k], pl.ds(own_rows, 128), :] = values[0:128]
        tokens[sources[k], pl.ds(other_rows, 128), :] = values[128:256]
        wide = values.astype(F32)
        square = square + jnp.sum(wide * wide, axis=1, keepdims=True)
    going = begin([(tokens, tokens_out)], semaphores.at[pl.ds(0, 1)])
    scale = lax.rsqrt(square * (1.0 / 1024.0) + EPSILON)
    normed = [
        (parts[k][...].astype(F32) * scale * gain_of(gain, sources[k])).astype(BF16)
        for k in range(4)
    ]
    starts = [pl.multiple_of(source * 256, 256) for source in sources]
    own_pad = pl.multiple_of(8 + core * 128, 8)
    other_pad = pl.multiple_of(8 + (1 - core) * 128, 8)
    a_pad = pl.multiple_of(core * 264, 8)
    b_pad = pl.multiple_of((1 - core) * 264, 8)
    for i in range(3):
        total = nn(normed[0], qkv_weight[i, pl.ds(starts[0], 256), :])
        for k in range(1, 4):
            total = total + nn(normed[k], qkv_weight[i, pl.ds(starts[k], 256), :])
        total = total.astype(BF16).astype(F32)
        columns = slice(i * 256, (i + 1) * 256)
        padded[pl.ds(own_pad, 128), columns] = total[0:128]
        padded[pl.ds(other_pad, 128), columns] = total[128:256]
        padded[pl.ds(a_pad, 8), columns] = total[256:264]
        padded[pl.ds(b_pad, 8), columns] = total[264:272]
    query[...] = padded[:, 0:256].astype(BF16)
    going += begin([(query, query_out)], semaphores.at[pl.ds(1, 1)])
    gate = nn(normed[0], gate_weight[pl.ds(starts[0], 256), :])
    for k in range(1, 4):
        gate = gate + nn(normed[k], gate_weight[pl.ds(starts[k], 256), :])
    own_extra = as_column(extra[pl.ds(core, 1), :])
    sent = extra_other[...].astype(F32)
    other_extra = as_column(sent[0:1, 0:128] + sent[0:1, 128:256] + sent[1:2, 0:128])
    decays = -2.0 * in_lanes(rate[...]) * jax.nn.sigmoid(gate[0:256])
    decay[pl.ds(own_rows, 128), :] = decays[0:128] - own_extra
    decay[pl.ds(other_rows, 128), :] = decays[128:256] - other_extra

    for i in (1, 2):
        columns = slice(i * 256, (i + 1) * 256)
        for direction in range(2):
            kv[direction, i - 1] = convolved(padded, taps, direction, i, columns)
    going += begin([(kv, kv_out)], semaphores.at[pl.ds(2, 1)])

    log_decay = decay[...]
    inflow = minus_expm1(log_decay)
    row, col = iota((ROWS, ROWS), 0), iota((ROWS, ROWS), 1)
    same = (row // SPAN) == (col // SPAN)
    earlier = (same & (col <= row)).astype(F32)
    later = (same & (col >= row)).astype(F32)
    spans = (iota((ROWS, 128 * SPANS), 0) // SPAN == iota((ROWS, 128 * SPANS), 1) // 128).astype(F32)
    for direction in range(2):
        cum[direction] = nn(later if direction else earlier, log_decay, HIGHEST)
        shrink[direction] = (jnp.exp(-cum[direction]) * inflow).astype(BF16)
    going += begin([(cum, cum_out), (shrink, shrink_out)], semaphores.at[pl.ds(3, 2)])
    span_totals = tn(log_decay, spans, HIGHEST)
    totals = [compact_rows(span_totals[:, n * 128 : (n + 1) * 128]) for n in range(SPANS)]
    factors = [jnp.exp(total) for total in totals]
    ends = []
    for direction in range(2):
        cumulative = cum[direction]
        states = [jnp.zeros((SPAN, LANES), F32), jnp.zeros((SPAN, LANES), F32)]
        passed = jnp.zeros((SPAN, LANES), F32)
        for n in reversed(range(SPANS)) if direction else range(SPANS):
            rows = slice(n * SPAN, (n + 1) * SPAN)
            start[direction, n, 0] = states[0].astype(BF16)
            start[direction, n, 1] = states[1].astype(BF16)
            reach[direction, n] = jnp.exp(passed)
            local = cumulative[rows]
            last = local[0:1] if direction else local[SPAN - 1 : SPAN]
            remain = (jnp.exp(last - local) * inflow[rows]).astype(BF16)
            for which in range(2):
                added = compact(tn(remain, kv[direction, which, rows, :]))
                states[which] = factors[n] * states[which] + added
            passed = passed + totals[n]
        ends.append(states)
    going += begin([(start, start_out), (reach, reach_out)], semaphores.at[pl.ds(5, 2)])
    factor = jnp.exp(totals[0] + totals[1] + totals[2] + totals[3])
    high = factor.astype(BF16).astype(F32)
    lane = iota((SPAN, LANES), 1)
    factor_parts = jnp.where(lane % 64 < 32, high, factor - high)
    for which in range(2):
        for half in range(2):
            lanes = slice(half * 128, (half + 1) * 128)
            for block in range(8):
                rows = slice(block * 8, block * 8 + 8)
                sent_out[which * 16 + half * 8 + block] = jnp.concatenate(
                    [
                        ends[0][which][rows, lanes],
                        ends[1][which][rows, lanes],
                        factor_parts[rows, lanes],
                    ],
                    axis=0,
                ).astype(BF16)
    finish(going)


def convolved(padded, taps, direction, i, columns):
    running = taps[direction, i, 0:1, :] * padded[8 : 8 + ROWS, columns]
    for j in range(1, 4):
        first = 8 + j if direction else 8 - j
        running = running + taps[direction, i, j : j + 1, :] * padded[first : first + ROWS, columns]
    return (running * jax.nn.sigmoid(running)).astype(BF16)


def own_head():
    return (iota((LANES, LANES), 0) // 64 == iota((LANES, LANES), 1) // 64).astype(BF16)


def expand(values, own):
    return jnp.concatenate([values] * 4, axis=0) * own


def seen_by(direction):
    position, other = iota((SPAN, LANES), 0), iota((SPAN, LANES), 1) % SPAN
    return other >= position if direction else other <= position


def meeting_kernel(
    query_in, kv_in, cum_in, shrink_in, start_in, taps,
    queries_out, scores_out, growth_out,
    query, keys, cum, shrink, start, padded, queries, scores, growth, semaphores,
):
    coming = begin(
        [
            (query_in, query),
            (kv_in.at[:, 0], keys),
            (cum_in, cum),
            (shrink_in, shrink),
            (start_in.at[:, :, 0], start),
        ],
        semaphores.at[pl.ds(0, 5)],
    )
    coming[0].wait()
    padded[...] = query[...].astype(F32)
    for direction in range(2):
        queries[direction] = convolved(padded, taps, direction, 0, slice(0, 256))
    going = begin([(queries, queries_out)], semaphores.at[pl.ds(5, 1)])
    finish(coming[1:])
    own = own_head()
    growth[...] = jnp.exp(cum[...])
    going += begin([(growth, growth_out)], semaphores.at[pl.ds(6, 1)])
    for n in range(SPANS):
        rows = slice(n * SPAN, (n + 1) * SPAN)
        for direction in range(2):
            asked = queries[direction, rows, :]
            meeting = nt(asked, expand(keys[direction, rows, :], own))
            meeting = jnp.where(seen_by(direction), meeting, 0.0).astype(BF16)
            scores[direction, rows, :] = growth[direction, rows, :] * (
                nn(meeting, expand(shrink[direction, rows, :], own))
                + nt(asked, expand(start[direction, n], own))
            )
    going += begin([(scores, scores_out)], semaphores.at[pl.ds(7, 1)])
    finish(going)


def scan_kernel(pieces, states_out, wide):
    count = pieces.shape[0]
    first = iota((8, 128), 1) % 64 < 32
    factors, forward, backward = [], [], []
    for i in range(count):
        piece = pieces[i].astype(F32)
        both = piece[16:24]
        factors.append(both + jnp.where(first, pltpu.roll(both, 96, 1), pltpu.roll(both, 32, 1)))
        forward.append(piece[0:8])
        backward.append(piece[8:16])
    state = jnp.zeros((8, 128), F32)
    for i in range(count):
        wide[i, 0:8, :] = state
        state = factors[i] * state + forward[i]
    state = jnp.zeros((8, 128), F32)
    for i in reversed(range(count)):
        wide[i, 8:16, :] = state
        state = factors[i] * state + backward[i]
    states_out[...] = wide[...].astype(BF16)


def head_max(values):
    first = in_first_head(SPAN)
    halves = []
    for half in range(2):
        part = values[:, half * 128 : (half + 1) * 128]
        left = jnp.max(jnp.where(first, part, -jnp.inf), axis=1, keepdims=True)
        right = jnp.max(jnp.where(first, -jnp.inf, part), axis=1, keepdims=True)
        halves.append(jnp.where(first, left, right))
    return jnp.concatenate(halves, axis=1)


def attention_kernel(
    queries_in, kv_in, shrink_in, start_in, reach_in, scores_in, growth_in, arrived, gain,
    out,
    queries, values, shrink, start, reach, scores, growth, entering, semaphores,
):
    coming = []
    for n in range(SPANS):
        rows = pl.ds(n * SPAN, SPAN)
        coming.append(
            begin(
                [
                    (reach_in.at[:, n], reach.at[:, n]),
                    (queries_in.at[:, rows, :], queries.at[:, rows, :]),
                    (growth_in.at[:, rows, :], growth.at[:, rows, :]),
                    (scores_in.at[:, rows, :], scores.at[:, rows, :]),
                    (shrink_in.at[:, rows, :], shrink.at[:, rows, :]),
                    (start_in.at[:, n, 1], start.at[:, n]),
                    (kv_in.at[:, 1, rows, :], values.at[:, rows, :]),
                ],
                semaphores.at[pl.ds(7 * n, 7)],
            )
        )
    for m in range(32):
        which, half, block = m // 16, (m // 8) % 2, m % 8
        piece = arrived[m].astype(F32)
        for direction in range(2):
            entering[direction, which, block * 8 : block * 8 + 8, half * 128 : half * 128 + 128] = (
                piece[direction * 8 : direction * 8 + 8]
            )
    own = own_head()
    gains = in_lanes(gain[...])
    for n in range(SPANS):
        finish(coming[n])
        rows = slice(n * SPAN, (n + 1) * SPAN)
        combined = jnp.zeros((SPAN, LANES), F32)
        for direction in range(2):
            lessen = expand(shrink[direction, rows, :], own)
            reached = reach[direction, n]
            grown = growth[direction, rows, :]
            key_state = expand((reached * entering[direction, 0]).astype(BF16), own)
            value_state = expand(
                (start[direction, n].astype(F32) + reached * entering[direction, 1]).astype(BF16),
                own,
            )
            total = scores[direction, rows, :] + grown * nt(queries[direction, rows, :], key_state)
            powers = jnp.exp(total - head_max(total))
            attend = powers / nn(powers.astype(BF16), own)
            weighted = (attend * grown).astype(BF16)
            mixing = jnp.where(seen_by(direction), nt(weighted, lessen), 0.0).astype(BF16)
            result = nn(mixing, expand(values[direction, rows, :], own)) + nn(weighted, value_state)
            mean = nn((result * result).astype(BF16), own) * (1.0 / 64.0)
            combined = combined + result * lax.rsqrt(mean + EPSILON) * gains
        out[rows, :] = combined.astype(BF16)


def tail_kernel(
    part0, part1, part2, part3, weight0, weight1, weight2, weight3, tokens_in, gain, up, down_in,
    base_out, out1, out2, out3, residual, update, tokens, down, semaphores,
):
    head = lax.axis_index("head")
    coming = begin([(tokens_in, tokens), (down_in, down)], semaphores)
    parts = (part0, part1, part2, part3)
    weights = (weight0, weight1, weight2, weight3)
    square = jnp.zeros((ROWS, 1), F32)
    for j in range(4):
        columns = slice(j * 256, (j + 1) * 256)
        total = nn(parts[0][...], weights[0][:, columns])
        for k in range(1, 4):
            total = total + nn(parts[k][...], weights[k][:, columns])
        if j == 0:
            coming[0].wait()
        value = (tokens[j].astype(F32) + total).astype(BF16).astype(F32)
        residual[j] = value
        square = square + jnp.sum(value * value, axis=1, keepdims=True)
    scale = lax.rsqrt(square * (1.0 / 1024.0) + EPSILON)
    entering = jnp.concatenate(
        [(residual[j] * scale * gain_of(gain, j)).astype(BF16) for j in range(4)], axis=1
    )
    hidden = jnp.concatenate(
        [
            jax.nn.gelu(nn(entering, up[:, j * 256 : (j + 1) * 256])).astype(BF16)
            for j in range(4)
        ],
        axis=1,
    )
    coming[1].wait()
    for j in range(4):
        update[j] = nn(hidden, down[:, j * 256 : (j + 1) * 256])
    base_out[...] = residual[head] + update[head]
    for k, out in ((1, out1), (2, out2), (3, out3)):
        out[...] = update[lax.rem(head + k, 4)].astype(BF16)


def finish_kernel(base, part1, part2, part3, kept_out, sent_out):
    core = lax.axis_index("core")

    def rows_of(which):
        rows = pl.ds(pl.multiple_of(which * 128, 128), 128)
        total = base[rows, :]
        for part in (part1, part2, part3):
            total = total + part[rows, :].astype(F32)
        return total.astype(BF16)

    kept_out[...] = rows_of(core)
    sent_out[...] = rows_of(1 - core)


def kernel(body, ins, outs, scratch=(), copies=0, flops=0):
    spaces = {"h": pltpu.HBM, "v": pltpu.VMEM}
    places = [pl.BlockSpec(memory_space=spaces[place]) for place in ins]
    shapes = [
        pltpu.HBM(out[0], out[1]) if out[2] == "h" else jax.ShapeDtypeStruct(out[0], out[1])
        for out in outs
    ]
    out_places = [pl.BlockSpec(memory_space=spaces[out[2]]) for out in outs]
    buffers = [pltpu.VMEM(shape, dtype) for shape, dtype in scratch]
    if copies:
        buffers.append(pltpu.SemaphoreType.DMA((copies,)))
    call = pl.pallas_call(
        body,
        in_specs=places,
        out_specs=out_places,
        out_shape=shapes,
        scratch_shapes=buffers,
        compiler_params=pltpu.CompilerParams(vmem_limit_bytes=32 * 1024 * 1024),
        cost_estimate=pl.CostEstimate(flops=flops, bytes_accessed=1 << 20, transcendentals=0),
    )

    def placed(*arrays):
        return call(
            *[
                pltpu.with_memory_space_constraint(array, pltpu.HBM) if place == "h" else array
                for array, place in zip(arrays, ins)
            ]
        )

    return placed


def shifted(value, k):
    count = lax.axis_size("head")
    return lax.ppermute(value, "head", [(j, (j + k) % count) for j in range(count)])


def local(
    tokens,
    input_norm_gain,
    query_key_value_weight,
    forget_gate_weight,
    convolution_filter_taps,
    slot_forget_rate,
    extra_forget_log,
    head_norm_gain,
    output_projection_weight,
    feedforward_norm_gain,
    up_projection_weight,
    down_projection_weight,
):
    chips = lax.axis_size(CHIPS)
    swap_pairs = [(0, 1), (1, 0)]
    swap, edge_a, edge_b, mine = kernel(
        split_kernel,
        "hh",
        [
            ((136, 256), BF16, "v"),
            ((8, 256), BF16, "v"),
            ((8, 256), BF16, "v"),
            ((128, 256), BF16, "v"),
        ],
        [((2, 128, 256), BF16), ((2, 128), F32)],
        copies=2,
    )(tokens, extra_forget_log)
    ahead = [(2 * i - 1, 2 * i) for i in range(1, chips)]
    behind = [(2 * i + 2, 2 * i + 1) for i in range(chips - 1)]
    other = lax.ppermute(swap, "core", swap_pairs)
    halo_a = lax.ppermute(edge_a, SEQ, ahead + behind)
    halo_b = lax.ppermute(
        edge_b,
        SEQ,
        [(2 * i - 1, 2 * i + 1) for i in range(1, chips)]
        + [(2 * i + 2, 2 * i) for i in range(chips - 1)],
    )
    rows = jnp.concatenate([mine, other[:128], halo_a, halo_b], axis=0)
    qkv_weight = jnp.transpose(query_key_value_weight, (1, 0, 2))
    rows, qkv_weight, gate_weight = lax.optimization_barrier(
        (rows, qkv_weight, forget_gate_weight)
    )
    parts = [rows] + [shifted(rows, k) for k in (1, 2, 3)]
    qkv_weight, gate_weight = kernel(
        warm_kernel,
        "hh",
        [((3, 1024, 256), BF16, "v"), ((1024, 256), BF16, "v")],
        copies=2,
        flops=10**9,
    )(qkv_weight, gate_weight)
    taps = jnp.transpose(convolution_filter_taps, (0, 2, 1, 3))
    halves = (2, ROWS, LANES)
    starts = (2, SPANS, 2, SPAN, LANES)
    reaches = (2, SPANS, SPAN, LANES)
    pieces, query, kv, cum, shrink, start, reach, whole_tokens = kernel(
        front_kernel,
        "v" * 11,
        [
            ((32, 24, 128), BF16, "v"),
            ((ROWS + 16, 256), BF16, "h"),
            ((2, 2, ROWS, LANES), BF16, "h"),
            (halves, F32, "h"),
            (halves, BF16, "h"),
            (starts, BF16, "h"),
            (reaches, F32, "h"),
            ((4, ROWS, 256), BF16, "h"),
        ],
        [
            ((ROWS + 16, 768), F32),
            ((ROWS, LANES), F32),
            ((ROWS + 16, 256), BF16),
            ((2, 2, ROWS, LANES), BF16),
            (halves, F32),
            (halves, BF16),
            (starts, BF16),
            (reaches, F32),
            ((4, ROWS, 256), BF16),
        ],
        copies=7,
        flops=10**9,
    )(
        *parts,
        input_norm_gain.reshape(8, 128),
        qkv_weight,
        gate_weight,
        taps,
        slot_forget_rate,
        extra_forget_log,
        other[128:],
    )
    pieces, out_weight = lax.optimization_barrier((pieces, output_projection_weight))
    out_weights = [out_weight] + [shifted(out_weight, k) for k in (1, 2, 3)]
    held = lax.all_to_all(pieces, CHIPS, split_axis=0, concat_axis=0, tiled=True)
    queries, scores, growth = kernel(
        meeting_kernel,
        "hhhhhv",
        [(halves, BF16, "h"), (halves, F32, "h"), (halves, F32, "h")],
        [
            ((ROWS + 16, 256), BF16),
            (halves, BF16),
            (halves, F32),
            (halves, BF16),
            (reaches, BF16),
            ((ROWS + 16, 256), F32),
            (halves, BF16),
            (halves, F32),
            (halves, F32),
        ],
        copies=8,
        flops=10**9,
    )(query, kv, cum, shrink, start, taps)
    (prefixes,) = kernel(
        scan_kernel, "v", [((chips, 16, 128), BF16, "v")], [((chips, 16, 128), F32)]
    )(held)
    arrived = lax.all_to_all(prefixes, CHIPS, split_axis=0, concat_axis=0, tiled=True)
    (attention,) = kernel(
        attention_kernel,
        "hhhhhhhvv",
        [((ROWS, LANES), BF16, "v")],
        [
            (halves, BF16),
            (halves, BF16),
            (halves, BF16),
            (reaches, BF16),
            (reaches, F32),
            (halves, F32),
            (halves, F32),
            ((2, 2, SPAN, LANES), F32),
        ],
        copies=28,
        flops=10**9,
    )(queries, kv, shrink, start, reach, scores, growth, arrived, head_norm_gain)
    attended = [attention] + [shifted(attention, k) for k in (1, 2, 3)]
    base, out1, out2, out3 = kernel(
        tail_kernel,
        "v" * 8 + "hvvh",
        [((ROWS, 256), F32, "v")] + [((ROWS, 256), BF16, "v")] * 3,
        [
            ((4, ROWS, 256), F32),
            ((4, ROWS, 256), F32),
            ((4, ROWS, 256), BF16),
            ((1024, 1024), BF16),
        ],
        copies=2,
        flops=2 * 10**9,
    )(
        *attended,
        *out_weights,
        whole_tokens,
        feedforward_norm_gain.reshape(8, 128),
        up_projection_weight,
        down_projection_weight,
    )
    kept, sent = kernel(
        finish_kernel, "vvvv", [((128, 256), BF16, "v"), ((128, 256), BF16, "v")]
    )(base, shifted(out1, 1), shifted(out2, 2), shifted(out3, 3))
    returned = lax.ppermute(sent, "core", swap_pairs)
    first = lax.axis_index("core") == 0
    return jnp.stack([jnp.where(first, kept, returned), jnp.where(first, returned, kept)])


def solution(mesh):
    split = Mesh(
        mesh.devices.reshape(4, 8, 2, mesh.shape["head"]), ("x", "z", "core", "head")
    )
    placed = (
        P(None, SEQ, "head"),
        P(),
        P(None, None, "head"),
        P(None, "head"),
        P(None, None, None, "head"),
        P("head", None),
        P(None, SEQ),
        P("head", None),
        P("head", None),
        P(),
        P(None, "head"),
        P("head", None),
    )
    return jax.shard_map(
        local, mesh=split, in_specs=placed, out_specs=P(None, SEQ, "head"), check_vma=False
    )
```

```python
import functools

import jax
import jax.numpy as jnp
from jax import lax
from jax.experimental import pallas as pl
from jax.experimental.pallas import tpu as pltpu
from jax.sharding import Mesh
from jax.sharding import PartitionSpec as P


CHIPS = ("x", "z")
SEQ = ("x", "z", "core")
EPSILON = 1e-06
BF16 = jnp.bfloat16
F32 = jnp.float32
HIGHEST = lax.Precision.HIGHEST
SPAN = 64
ROWS = 256
LANES = 256
SPANS = ROWS // SPAN


def nn(a, b, precision=None):
    return lax.dot_general(
        a, b, (((1,), (0,)), ((), ())), preferred_element_type=F32, precision=precision
    )


def nt(a, b):
    return lax.dot_general(a, b, (((1,), (1,)), ((), ())), preferred_element_type=F32)


def tn(a, b, precision=None):
    return lax.dot_general(
        a, b, (((0,), (0,)), ((), ())), preferred_element_type=F32, precision=precision
    )


def iota(shape, dim):
    return lax.broadcasted_iota(jnp.int32, shape, dim)


def in_first_head(rows):
    return iota((rows, 128), 1) < 64


def compact(blocks):
    first = in_first_head(64)
    left = jnp.where(first, blocks[0:64, 0:128], blocks[64:128, 0:128])
    right = jnp.where(first, blocks[128:192, 128:256], blocks[192:256, 128:256])
    return jnp.concatenate([left, right], axis=1)


def compact_rows(column):
    first = in_first_head(64)
    left = jnp.where(first, column[0:64], column[64:128])
    right = jnp.where(first, column[128:192], column[192:256])
    return jnp.concatenate([left, right], axis=1)


def minus_expm1(x):
    series = 1.0 + x * (1.0 / 7.0)
    for k in (6, 5, 4, 3, 2):
        series = 1.0 + x * (1.0 / k) * series
    return jnp.where(x > -0.3, -x * series, 1.0 - jnp.exp(x))


def as_column(row):
    picked = jnp.where(iota((128, 128), 0) == iota((128, 128), 1), row, 0.0)
    return jnp.sum(picked, axis=1, keepdims=True)


def begin(pairs, semaphores):
    copies = [
        pltpu.make_async_copy(source, target, semaphores.at[k])
        for k, (source, target) in enumerate(pairs)
    ]
    for copy in copies:
        copy.start()
    return copies


def finish(copies):
    for copy in copies:
        copy.wait()


def in_lanes(heads):
    return jnp.concatenate([heads[h : h + 1, :] for h in range(4)], axis=1)


def gain_of(gain, source):
    return jnp.concatenate(
        [gain[pl.ds(2 * source, 1), :], gain[pl.ds(2 * source + 1, 1), :]], axis=1
    )


def warm_kernel(qkv_weight, gate_weight, qkv_out, gate_out, semaphores):
    finish(begin([(qkv_weight, qkv_out), (gate_weight, gate_out)], semaphores))


def edge_kernel(tokens_in, extra_in, edge_out, swap_out, mine_out, tokens, extra, semaphores):
    core = lax.axis_index("core")
    finish(begin([(tokens_in, tokens), (extra_in, extra)], semaphores))
    mine_out[...] = tokens[core]
    for which in range(2):
        wide = tokens[which].astype(F32)
        edge_out[which] = jnp.where(core == 1, wide[120:128], wide[0:8]).astype(BF16)
    row = extra[pl.ds(1 - core, 1), :]
    high = row.astype(BF16).astype(F32)
    middle = (row - high).astype(BF16).astype(F32)
    low = row - high - middle
    line = iota((8, 256), 0)
    first = jnp.concatenate([high, middle], axis=1)
    second = jnp.concatenate([low, low], axis=1)
    packed = jnp.where(line == 0, first, jnp.where(line == 1, second, 0.0))
    swap_out[0:128] = tokens[1 - core]
    swap_out[128:136] = packed.astype(BF16)


def swap_kernel(local_part, edges, swap_out, kept_out):
    core = lax.axis_index("core")
    swap_out[0:136] = local_part[...]
    swap_out[136:144] = edges[1 - core]
    kept_out[...] = edges[core]


def front_kernel(
    part0, part1, part2, part3, gain, qkv_weight, gate_weight, taps, rate, extra, extra_other,
    sent_out, query_out, kv_out, cum_out, shrink_out, start_out, reach_out, kept_out, passed_out,
    padded, decay, query, kv, cum, shrink, start, reach, kept, passed_on, semaphores,
):
    core = lax.axis_index("core")
    head = lax.axis_index("head")
    parts = (part0, part1, part2, part3)
    sources = [lax.rem(head + 4 - k, 4) for k in range(4)]
    own_rows = pl.multiple_of(core * 128, 128)
    other_rows = pl.multiple_of((1 - core) * 128, 128)
    square = jnp.zeros((ROWS + 16, 1), F32)
    for k in range(4):
        values = parts[k][...]
        kept[sources[k]] = values[0:128]
        passed_on[sources[k]] = values[128:256]
        wide = values.astype(F32)
        square = square + jnp.sum(wide * wide, axis=1, keepdims=True)
    going = begin([(kept, kept_out), (passed_on, passed_out)], semaphores.at[pl.ds(0, 2)])
    scale = lax.rsqrt(square * (1.0 / 1024.0) + EPSILON)
    normed = [
        (parts[k][...].astype(F32) * scale * gain_of(gain, sources[k])).astype(BF16)
        for k in range(4)
    ]
    starts = [pl.multiple_of(source * 256, 256) for source in sources]
    own_pad = pl.multiple_of(8 + core * 128, 8)
    other_pad = pl.multiple_of(8 + (1 - core) * 128, 8)
    a_pad = pl.multiple_of(core * 264, 8)
    b_pad = pl.multiple_of((1 - core) * 264, 8)
    for i in range(3):
        total = nn(normed[0], qkv_weight[i, pl.ds(starts[0], 256), :])
        for k in range(1, 4):
            total = total + nn(normed[k], qkv_weight[i, pl.ds(starts[k], 256), :])
        total = total.astype(BF16).astype(F32)
        columns = slice(i * 256, (i + 1) * 256)
        padded[pl.ds(own_pad, 128), columns] = total[0:128]
        padded[pl.ds(other_pad, 128), columns] = total[128:256]
        padded[pl.ds(a_pad, 8), columns] = total[256:264]
        padded[pl.ds(b_pad, 8), columns] = total[264:272]
    query[...] = padded[:, 0:256].astype(BF16)
    going += begin([(query, query_out)], semaphores.at[pl.ds(2, 1)])
    gate = nn(normed[0], gate_weight[pl.ds(starts[0], 256), :])
    for k in range(1, 4):
        gate = gate + nn(normed[k], gate_weight[pl.ds(starts[k], 256), :])
    own_extra = as_column(extra[pl.ds(core, 1), :])
    sent = extra_other[...].astype(F32)
    other_extra = as_column(sent[0:1, 0:128] + sent[0:1, 128:256] + sent[1:2, 0:128])
    decays = -2.0 * in_lanes(rate[...]) * jax.nn.sigmoid(gate[0:256])
    decay[pl.ds(own_rows, 128), :] = decays[0:128] - own_extra
    decay[pl.ds(other_rows, 128), :] = decays[128:256] - other_extra

    for i in (1, 2):
        columns = slice(i * 256, (i + 1) * 256)
        for direction in range(2):
            kv[direction, i - 1] = convolved(padded, taps, direction, i, columns)
    going += begin([(kv, kv_out)], semaphores.at[pl.ds(3, 1)])

    log_decay = decay[...]
    inflow = minus_expm1(log_decay)
    row, col = iota((ROWS, ROWS), 0), iota((ROWS, ROWS), 1)
    same = (row // SPAN) == (col // SPAN)
    earlier = (same & (col <= row)).astype(F32)
    later = (same & (col >= row)).astype(F32)
    spans = (iota((ROWS, 128 * SPANS), 0) // SPAN == iota((ROWS, 128 * SPANS), 1) // 128).astype(F32)
    for direction in range(2):
        cum[direction] = nn(later if direction else earlier, log_decay, HIGHEST)
        shrink[direction] = (jnp.exp(-cum[direction]) * inflow).astype(BF16)
    going += begin([(cum, cum_out), (shrink, shrink_out)], semaphores.at[pl.ds(4, 2)])
    span_totals = tn(log_decay, spans, HIGHEST)
    totals = [compact_rows(span_totals[:, n * 128 : (n + 1) * 128]) for n in range(SPANS)]
    factors = [jnp.exp(total) for total in totals]
    ends = []
    for direction in range(2):
        cumulative = cum[direction]
        states = [jnp.zeros((SPAN, LANES), F32), jnp.zeros((SPAN, LANES), F32)]
        passed = jnp.zeros((SPAN, LANES), F32)
        for n in reversed(range(SPANS)) if direction else range(SPANS):
            rows = slice(n * SPAN, (n + 1) * SPAN)
            start[direction, n, 0] = states[0].astype(BF16)
            start[direction, n, 1] = states[1].astype(BF16)
            reach[direction, n] = jnp.exp(passed)
            local = cumulative[rows]
            last = local[0:1] if direction else local[SPAN - 1 : SPAN]
            remain = (jnp.exp(last - local) * inflow[rows]).astype(BF16)
            for which in range(2):
                added = compact(tn(remain, kv[direction, which, rows, :]))
                states[which] = factors[n] * states[which] + added
            passed = passed + totals[n]
        ends.append(states)
    going += begin([(start, start_out), (reach, reach_out)], semaphores.at[pl.ds(6, 2)])
    factor = jnp.exp(totals[0] + totals[1] + totals[2] + totals[3])
    high = factor.astype(BF16).astype(F32)
    lane = iota((SPAN, LANES), 1)
    factor_parts = jnp.where(lane % 64 < 32, high, factor - high)
    for which in range(2):
        for half in range(2):
            lanes = slice(half * 128, (half + 1) * 128)
            for block in range(8):
                rows = slice(block * 8, block * 8 + 8)
                sent_out[which * 16 + half * 8 + block] = jnp.concatenate(
                    [
                        ends[0][which][rows, lanes],
                        ends[1][which][rows, lanes],
                        factor_parts[rows, lanes],
                    ],
                    axis=0,
                ).astype(BF16)
    finish(going)


def convolved(padded, taps, direction, i, columns):
    running = taps[direction, i, 0:1, :] * padded[8 : 8 + ROWS, columns]
    for j in range(1, 4):
        first = 8 + j if direction else 8 - j
        running = running + taps[direction, i, j : j + 1, :] * padded[first : first + ROWS, columns]
    return (running * jax.nn.sigmoid(running)).astype(BF16)


def own_head():
    return (iota((LANES, LANES), 0) // 64 == iota((LANES, LANES), 1) // 64).astype(BF16)


def expand(values, own):
    return jnp.concatenate([values] * 4, axis=0) * own


def seen_by(direction):
    position, other = iota((SPAN, LANES), 0), iota((SPAN, LANES), 1) % SPAN
    return other >= position if direction else other <= position


def meeting_kernel(
    query_in, kv_in, cum_in, shrink_in, start_in, taps,
    queries_out, scores_out, growth_out,
    query, keys, cum, shrink, start, padded, queries, scores, growth, semaphores,
):
    coming = begin(
        [
            (query_in, query),
            (kv_in.at[:, 0], keys),
            (cum_in, cum),
            (shrink_in, shrink),
            (start_in.at[:, :, 0], start),
        ],
        semaphores.at[pl.ds(0, 5)],
    )
    coming[0].wait()
    padded[...] = query[...].astype(F32)
    for direction in range(2):
        queries[direction] = convolved(padded, taps, direction, 0, slice(0, 256))
    going = begin([(queries, queries_out)], semaphores.at[pl.ds(5, 1)])
    finish(coming[1:])
    own = own_head()
    growth[...] = jnp.exp(cum[...])
    going += begin([(growth, growth_out)], semaphores.at[pl.ds(6, 1)])
    for n in range(SPANS):
        rows = slice(n * SPAN, (n + 1) * SPAN)
        for direction in range(2):
            asked = queries[direction, rows, :]
            meeting = nt(asked, expand(keys[direction, rows, :], own))
            meeting = jnp.where(seen_by(direction), meeting, 0.0).astype(BF16)
            scores[direction, rows, :] = growth[direction, rows, :] * (
                nn(meeting, expand(shrink[direction, rows, :], own))
                + nt(asked, expand(start[direction, n], own))
            )
    going += begin([(scores, scores_out)], semaphores.at[pl.ds(7, 1)])
    finish(going)


def scan_kernel(pieces, states_out, wide):
    count = pieces.shape[0]
    first = iota((8, 128), 1) % 64 < 32
    factors, forward, backward = [], [], []
    for i in range(count):
        piece = pieces[i].astype(F32)
        both = piece[16:24]
        factors.append(both + jnp.where(first, pltpu.roll(both, 96, 1), pltpu.roll(both, 32, 1)))
        forward.append(piece[0:8])
        backward.append(piece[8:16])
    state = jnp.zeros((8, 128), F32)
    for i in range(count):
        wide[i, 0:8, :] = state
        state = factors[i] * state + forward[i]
    state = jnp.zeros((8, 128), F32)
    for i in reversed(range(count)):
        wide[i, 8:16, :] = state
        state = factors[i] * state + backward[i]
    states_out[...] = wide[...].astype(BF16)


def head_max(values):
    first = in_first_head(values.shape[0])
    halves = []
    for half in range(2):
        part = values[:, half * 128 : (half + 1) * 128]
        left = jnp.max(jnp.where(first, part, -jnp.inf), axis=1, keepdims=True)
        right = jnp.max(jnp.where(first, -jnp.inf, part), axis=1, keepdims=True)
        halves.append(jnp.where(first, left, right))
    return jnp.concatenate(halves, axis=1)


def attention_kernel(
    own_half,
    queries_in, kv_in, shrink_in, start_in, reach_in, scores_in, growth_in, arrived, gain,
    out,
    queries, values, shrink, start, reach, scores, growth, weighted, mixing, result, entering,
    semaphores,
):
    core = lax.axis_index("core")
    half_index = core if own_half else 1 - core
    rows = pl.ds(pl.multiple_of(half_index * 128, 128), 128)
    spans = pl.ds(half_index * 2, 2)
    coming = begin(
        [
            (reach_in.at[:, spans], reach),
            (queries_in.at[:, rows, :], queries),
            (growth_in.at[:, rows, :], growth),
            (scores_in.at[:, rows, :], scores),
            (shrink_in.at[:, rows, :], shrink),
            (start_in.at[:, spans, 1], start),
            (kv_in.at[:, 1, rows, :], values),
        ],
        semaphores,
    )
    for m in range(32):
        which, half, block = m // 16, (m // 8) % 2, m % 8
        piece = arrived[m].astype(F32)
        for direction in range(2):
            entering[direction, which, block * 8 : block * 8 + 8, half * 128 : half * 128 + 128] = (
                piece[direction * 8 : direction * 8 + 8]
            )
    own = own_head()
    gains = in_lanes(gain[...])
    units = [(direction, n) for direction in range(2) for n in range(2)]
    finish(coming[:4])
    for direction, n in units:
        span = slice(n * SPAN, (n + 1) * SPAN)
        key_state = expand((reach[direction, n] * entering[direction, 0]).astype(BF16), own)
        scores[direction, span, :] = scores[direction, span, :] + growth[
            direction, span, :
        ] * nt(queries[direction, span, :], key_state)
    for direction in range(2):
        total = scores[direction]
        powers = jnp.exp(total - head_max(total))
        attend = powers / nn(powers.astype(BF16), own)
        weighted[direction] = (attend * growth[direction]).astype(BF16)
    finish(coming[4:])
    for direction, n in units:
        span = slice(n * SPAN, (n + 1) * SPAN)
        lessen = expand(shrink[direction, span, :], own)
        mixed = jnp.where(seen_by(direction), nt(weighted[direction, span, :], lessen), 0.0)
        mixing[direction, span, :] = mixed.astype(BF16)
    for direction, n in units:
        span = slice(n * SPAN, (n + 1) * SPAN)
        state = start[direction, n].astype(F32) + reach[direction, n] * entering[direction, 1]
        result[direction, span, :] = nn(
            mixing[direction, span, :], expand(values[direction, span, :], own)
        ) + nn(weighted[direction, span, :], expand(state.astype(BF16), own))
    combined = jnp.zeros((128, LANES), F32)
    for direction in range(2):
        found = result[direction]
        mean = nn((found * found).astype(BF16), own) * (1.0 / 64.0)
        combined = combined + found * lax.rsqrt(mean + EPSILON) * gains
    out[...] = combined.astype(BF16)


def tail_kernel(
    part0, part1, part2, part3, weight0, weight1, weight2, weight3, kept_in, passed_in, gain, up, down_in,
    base_out, out1, out2, out3, residual, update, tokens, down, semaphores,
):
    head = lax.axis_index("head")
    coming = begin(
        [(kept_in, tokens.at[:, 0:128]), (passed_in, tokens.at[:, 128:256]), (down_in, down)],
        semaphores,
    )
    parts = (part0, part1, part2, part3)
    weights = (weight0, weight1, weight2, weight3)
    square = jnp.zeros((ROWS, 1), F32)
    for j in range(4):
        columns = slice(j * 256, (j + 1) * 256)
        total = nn(parts[0][...], weights[0][:, columns])
        for k in range(1, 4):
            total = total + nn(parts[k][...], weights[k][:, columns])
        if j == 0:
            finish(coming[:2])
        value = (tokens[j].astype(F32) + total).astype(BF16).astype(F32)
        residual[j] = value
        square = square + jnp.sum(value * value, axis=1, keepdims=True)
    scale = lax.rsqrt(square * (1.0 / 1024.0) + EPSILON)
    entering = jnp.concatenate(
        [(residual[j] * scale * gain_of(gain, j)).astype(BF16) for j in range(4)], axis=1
    )
    hidden = jnp.concatenate(
        [
            jax.nn.gelu(nn(entering, up[:, j * 256 : (j + 1) * 256])).astype(BF16)
            for j in range(4)
        ],
        axis=1,
    )
    coming[2].wait()
    for j in range(4):
        update[j] = nn(hidden, down[:, j * 256 : (j + 1) * 256])
    base_out[...] = residual[head] + update[head]
    for k, out in ((1, out1), (2, out2), (3, out3)):
        out[...] = update[lax.rem(head + k, 4)].astype(BF16)


def finish_kernel(base, part1, part2, part3, out):
    core = lax.axis_index("core")
    total = base[...]
    for part in (part1, part2, part3):
        total = total + part[...].astype(F32)
    total = total.astype(BF16)
    out[core] = total[0:128]
    out[1 - core] = total[128:256]


def kernel(body, ins, outs, scratch=(), copies=0, flops=0):
    spaces = {"h": pltpu.HBM, "v": pltpu.VMEM}
    places = [pl.BlockSpec(memory_space=spaces[place]) for place in ins]
    shapes = [
        pltpu.HBM(out[0], out[1]) if out[2] == "h" else jax.ShapeDtypeStruct(out[0], out[1])
        for out in outs
    ]
    out_places = [pl.BlockSpec(memory_space=spaces[out[2]]) for out in outs]
    buffers = [pltpu.VMEM(shape, dtype) for shape, dtype in scratch]
    if copies:
        buffers.append(pltpu.SemaphoreType.DMA((copies,)))
    call = pl.pallas_call(
        body,
        in_specs=places,
        out_specs=out_places,
        out_shape=shapes,
        scratch_shapes=buffers,
        compiler_params=pltpu.CompilerParams(vmem_limit_bytes=32 * 1024 * 1024),
        cost_estimate=pl.CostEstimate(flops=flops, bytes_accessed=1 << 20, transcendentals=0),
    )

    def placed(*arrays):
        return call(
            *[
                pltpu.with_memory_space_constraint(array, pltpu.HBM) if place == "h" else array
                for array, place in zip(arrays, ins)
            ]
        )

    return placed


def shifted(value, k):
    count = lax.axis_size("head")
    return lax.ppermute(value, "head", [(j, (j + k) % count) for j in range(count)])


def local(
    tokens,
    input_norm_gain,
    query_key_value_weight,
    forget_gate_weight,
    convolution_filter_taps,
    slot_forget_rate,
    extra_forget_log,
    head_norm_gain,
    output_projection_weight,
    feedforward_norm_gain,
    up_projection_weight,
    down_projection_weight,
):
    chips = lax.axis_size(CHIPS)
    swap_pairs = [(0, 1), (1, 0)]
    edges, swap, mine = kernel(
        edge_kernel,
        "hh",
        [((2, 8, 256), BF16, "v"), ((136, 256), BF16, "v"), ((128, 256), BF16, "v")],
        [((2, 128, 256), BF16), ((2, 128), F32)],
        copies=2,
    )(tokens, extra_forget_log)
    ahead = [(2 * i - 1, 2 * i) for i in range(1, chips)]
    behind = [(2 * i + 2, 2 * i + 1) for i in range(chips - 1)]
    edges = lax.ppermute(edges, SEQ, ahead + behind)
    swap, kept_edge = kernel(
        swap_kernel, "vv", [((144, 256), BF16, "v"), ((8, 256), BF16, "v")]
    )(swap, edges)
    other = lax.ppermute(swap, "core", swap_pairs)
    rows = jnp.concatenate([mine, other[:128], kept_edge, other[136:]], axis=0)
    qkv_weight = jnp.transpose(query_key_value_weight, (1, 0, 2))
    rows, qkv_weight, gate_weight = lax.optimization_barrier(
        (rows, qkv_weight, forget_gate_weight)
    )
    parts = [rows] + [shifted(rows, k) for k in (1, 2, 3)]
    qkv_weight, gate_weight = kernel(
        warm_kernel,
        "hh",
        [((3, 1024, 256), BF16, "v"), ((1024, 256), BF16, "v")],
        copies=2,
        flops=10**9,
    )(qkv_weight, gate_weight)
    taps = jnp.transpose(convolution_filter_taps, (0, 2, 1, 3))
    halves = (2, ROWS, LANES)
    starts = (2, SPANS, 2, SPAN, LANES)
    reaches = (2, SPANS, SPAN, LANES)
    pieces, query, kv, cum, shrink, start, reach, kept, passed = kernel(
        front_kernel,
        "v" * 11,
        [
            ((32, 24, 128), BF16, "v"),
            ((ROWS + 16, 256), BF16, "h"),
            ((2, 2, ROWS, LANES), BF16, "h"),
            (halves, F32, "h"),
            (halves, BF16, "h"),
            (starts, BF16, "h"),
            (reaches, F32, "h"),
            ((4, 128, 256), BF16, "h"),
            ((4, 128, 256), BF16, "h"),
        ],
        [
            ((ROWS + 16, 768), F32),
            ((ROWS, LANES), F32),
            ((ROWS + 16, 256), BF16),
            ((2, 2, ROWS, LANES), BF16),
            (halves, F32),
            (halves, BF16),
            (starts, BF16),
            (reaches, F32),
            ((4, 128, 256), BF16),
            ((4, 128, 256), BF16),
        ],
        copies=8,
        flops=10**9,
    )(
        *parts,
        input_norm_gain.reshape(8, 128),
        qkv_weight,
        gate_weight,
        taps,
        slot_forget_rate,
        extra_forget_log,
        other[128:136],
    )
    pieces, out_weight, passed = lax.optimization_barrier(
        (pieces, output_projection_weight, passed)
    )
    held = lax.all_to_all(pieces, CHIPS, split_axis=0, concat_axis=0, tiled=True)
    out_weights = [out_weight]
    for k in (1, 2, 3):
        out_weights.append(shifted(out_weight, k))
    passed = lax.ppermute(passed, "core", swap_pairs)
    meeting = kernel(
        meeting_kernel,
        "hhhhhv",
        [(halves, BF16, "h"), (halves, F32, "h"), (halves, F32, "h")],
        [
            ((ROWS + 16, 256), BF16),
            (halves, BF16),
            (halves, F32),
            (halves, BF16),
            (reaches, BF16),
            ((ROWS + 16, 256), F32),
            (halves, BF16),
            (halves, F32),
            (halves, F32),
        ],
        copies=8,
        flops=10**9,
    )
    queries, scores, growth = meeting(query, kv, cum, shrink, start, taps)
    (prefixes,) = kernel(
        scan_kernel, "v", [((chips, 16, 128), BF16, "v")], [((chips, 16, 128), F32)]
    )(held)
    arrived = lax.all_to_all(prefixes, CHIPS, split_axis=0, concat_axis=0, tiled=True)
    half = (2, 128, LANES)
    reached = (2, 2, SPAN, LANES)
    attention = []
    for own_half in (False, True):
        attend = kernel(
            functools.partial(attention_kernel, own_half),
            "hhhhhhhvv",
            [((128, LANES), BF16, "v")],
            [
                (half, BF16),
                (half, BF16),
                (half, BF16),
                (reached, BF16),
                (reached, F32),
                (half, F32),
                (half, F32),
                (half, BF16),
                (half, BF16),
                (half, F32),
                ((2, 2, SPAN, LANES), F32),
            ],
            copies=7,
            flops=10**9,
        )
        attention += attend(
            queries, kv, shrink, start, reach, scores, growth, arrived, head_norm_gain
        )
    swapped = lax.ppermute(attention[0], "core", swap_pairs)
    attention = jnp.concatenate([attention[1], swapped], axis=0)
    attended = [attention] + [shifted(attention, k) for k in (1, 2, 3)]
    base, out1, out2, out3 = kernel(
        tail_kernel,
        "v" * 8 + "hhvvh",
        [((ROWS, 256), F32, "v")] + [((ROWS, 256), BF16, "v")] * 3,
        [
            ((4, ROWS, 256), F32),
            ((4, ROWS, 256), F32),
            ((4, ROWS, 256), BF16),
            ((1024, 1024), BF16),
        ],
        copies=3,
        flops=2 * 10**9,
    )(
        *attended,
        *out_weights,
        kept,
        passed,
        feedforward_norm_gain.reshape(8, 128),
        up_projection_weight,
        down_projection_weight,
    )
    (out,) = kernel(finish_kernel, "vvvv", [((2, 128, 256), BF16, "v")])(
        base, shifted(out1, 1), shifted(out2, 2), shifted(out3, 3)
    )
    return out


def solution(mesh):
    split = Mesh(
        mesh.devices.reshape(4, 8, 2, mesh.shape["head"]), ("x", "z", "core", "head")
    )
    placed = (
        P(None, SEQ, "head"),
        P(),
        P(None, None, "head"),
        P(None, "head"),
        P(None, None, None, "head"),
        P("head", None),
        P(None, SEQ),
        P("head", None),
        P("head", None),
        P(),
        P(None, "head"),
        P("head", None),
    )

    return jax.shard_map(
        local, mesh=split, in_specs=placed, out_specs=P(None, SEQ, "head"), check_vma=False
    )
```

```python
import functools

import jax
import jax.numpy as jnp
from jax import lax
from jax.experimental import pallas as pl
from jax.experimental.pallas import tpu as pltpu
from jax.sharding import Mesh
from jax.sharding import PartitionSpec as P


CHIPS = ("x", "z")
SEQ = ("x", "z", "core")
EPSILON = 1e-06
BF16 = jnp.bfloat16
F32 = jnp.float32
SPAN = 64
ROWS = 256
LANES = 256
SPANS = ROWS // SPAN


def nn(a, b, precision=None):
    return lax.dot_general(
        a, b, (((1,), (0,)), ((), ())), preferred_element_type=F32, precision=precision
    )


def nt(a, b):
    return lax.dot_general(a, b, (((1,), (1,)), ((), ())), preferred_element_type=F32)


def tn(a, b, precision=None):
    return lax.dot_general(
        a, b, (((0,), (0,)), ((), ())), preferred_element_type=F32, precision=precision
    )


def iota(shape, dim):
    return lax.broadcasted_iota(jnp.int32, shape, dim)


def in_first_head(rows):
    return iota((rows, 128), 1) < 64


def compact(blocks):
    first = in_first_head(64)
    left = jnp.where(first, blocks[0:64, 0:128], blocks[64:128, 0:128])
    right = jnp.where(first, blocks[128:192, 128:256], blocks[192:256, 128:256])
    return jnp.concatenate([left, right], axis=1)


def compact_rows(column):
    first = in_first_head(64)
    left = jnp.where(first, column[0:64], column[64:128])
    right = jnp.where(first, column[128:192], column[192:256])
    return jnp.concatenate([left, right], axis=1)


def minus_expm1(x):
    series = 1.0 + x * (1.0 / 7.0)
    for k in (6, 5, 4, 3, 2):
        series = 1.0 + x * (1.0 / k) * series
    return jnp.where(x > -0.3, -x * series, 1.0 - jnp.exp(x))


def exact(matmul, values, zeros_and_ones):
    high = values.astype(BF16)
    rest = values - high.astype(F32)
    middle = rest.astype(BF16)
    low = (rest - middle.astype(F32)).astype(BF16)
    return (
        matmul(low, zeros_and_ones) + matmul(middle, zeros_and_ones)
    ) + matmul(high, zeros_and_ones)


def as_column(row):
    picked = jnp.where(iota((128, 128), 0) == iota((128, 128), 1), row, 0.0)
    return jnp.sum(picked, axis=1, keepdims=True)


def begin(pairs, semaphores):
    copies = [
        pltpu.make_async_copy(source, target, semaphores.at[k])
        for k, (source, target) in enumerate(pairs)
    ]
    for copy in copies:
        copy.start()
    return copies


def finish(copies):
    for copy in copies:
        copy.wait()


def in_lanes(heads):
    return jnp.concatenate([heads[h : h + 1, :] for h in range(4)], axis=1)


def gain_of(gain, source):
    return jnp.concatenate(
        [gain[pl.ds(2 * source, 1), :], gain[pl.ds(2 * source + 1, 1), :]], axis=1
    )


def warm_kernel(qkv_weight, gate_weight, out_weight, qkv_out, gate_out, half_out, semaphores):
    rows = pl.ds(pl.multiple_of(lax.axis_index("core") * 128, 128), 128)
    finish(
        begin(
            [
                (qkv_weight, qkv_out),
                (gate_weight, gate_out),
                (out_weight.at[rows, :], half_out),
            ],
            semaphores,
        )
    )


def warm_tail_kernel(
    weight0, mine1, mine2, mine3, theirs1, theirs2, theirs3, kept, passed, down,
    weights_out, tokens_out, down_out, semaphores,
):
    core = lax.axis_index("core")
    own = pl.ds(pl.multiple_of(core * 128, 128), 128)
    other = pl.ds(pl.multiple_of((1 - core) * 128, 128), 128)
    pairs = [(weight0, weights_out.at[0])]
    for k, mine, theirs in ((1, mine1, theirs1), (2, mine2, theirs2), (3, mine3, theirs3)):
        pairs += [(mine, weights_out.at[k, own]), (theirs, weights_out.at[k, other])]
    pairs += [(kept, tokens_out.at[:, 0:128]), (passed, tokens_out.at[:, 128:256])]
    finish(begin(pairs + [(down, down_out)], semaphores))


def edge_kernel(tokens_in, extra_in, edge_out, swap_out, mine_out, tokens, extra, semaphores):
    core = lax.axis_index("core")
    finish(begin([(tokens_in, tokens), (extra_in, extra)], semaphores))
    mine_out[...] = tokens[core]
    for which in range(2):
        wide = tokens[which].astype(F32)
        edge_out[which] = jnp.where(core == 1, wide[120:128], wide[0:8]).astype(BF16)
    row = extra[pl.ds(1 - core, 1), :]
    high = row.astype(BF16).astype(F32)
    middle = (row - high).astype(BF16).astype(F32)
    low = row - high - middle
    line = iota((8, 256), 0)
    first = jnp.concatenate([high, middle], axis=1)
    second = jnp.concatenate([low, low], axis=1)
    packed = jnp.where(line == 0, first, jnp.where(line == 1, second, 0.0))
    swap_out[0:128] = tokens[1 - core]
    swap_out[128:136] = packed.astype(BF16)


def swap_kernel(local_part, edges, swap_out, kept_out):
    core = lax.axis_index("core")
    swap_out[0:136] = local_part[...]
    swap_out[136:144] = edges[1 - core]
    kept_out[...] = edges[core]


def front_kernel(
    part0, part1, part2, part3, gain, qkv_weight, gate_weight, taps, rate, extra, extra_other,
    sent_out, query_out, kv_out, cum_out, shrink_out, start_out, reach_out, kept_out, passed_out,
    padded, decay, query, kv, cum, shrink, start, reach, kept, passed_on, semaphores,
):
    core = lax.axis_index("core")
    head = lax.axis_index("head")
    parts = (part0, part1, part2, part3)
    sources = [lax.rem(head + 4 - k, 4) for k in range(4)]
    own_rows = pl.multiple_of(core * 128, 128)
    other_rows = pl.multiple_of((1 - core) * 128, 128)
    square = jnp.zeros((ROWS + 16, 1), F32)
    for k in range(4):
        values = parts[k][...]
        kept[sources[k]] = values[0:128]
        passed_on[sources[k]] = values[128:256]
        wide = values.astype(F32)
        square = square + jnp.sum(wide * wide, axis=1, keepdims=True)
    going = begin([(kept, kept_out), (passed_on, passed_out)], semaphores.at[pl.ds(0, 2)])
    scale = lax.rsqrt(square * (1.0 / 1024.0) + EPSILON)
    normed = [
        (parts[k][...].astype(F32) * scale * gain_of(gain, sources[k])).astype(BF16)
        for k in range(4)
    ]
    starts = [pl.multiple_of(source * 256, 256) for source in sources]
    own_pad = pl.multiple_of(8 + core * 128, 8)
    other_pad = pl.multiple_of(8 + (1 - core) * 128, 8)
    a_pad = pl.multiple_of(core * 264, 8)
    b_pad = pl.multiple_of((1 - core) * 264, 8)
    for i in range(3):
        total = nn(normed[0], qkv_weight[i, pl.ds(starts[0], 256), :])
        for k in range(1, 4):
            total = total + nn(normed[k], qkv_weight[i, pl.ds(starts[k], 256), :])
        total = total.astype(BF16).astype(F32)
        columns = slice(i * 256, (i + 1) * 256)
        padded[pl.ds(own_pad, 128), columns] = total[0:128]
        padded[pl.ds(other_pad, 128), columns] = total[128:256]
        padded[pl.ds(a_pad, 8), columns] = total[256:264]
        padded[pl.ds(b_pad, 8), columns] = total[264:272]
    query[...] = padded[:, 0:256].astype(BF16)
    going += begin([(query, query_out)], semaphores.at[pl.ds(2, 1)])
    gate = nn(normed[0], gate_weight[pl.ds(starts[0], 256), :])
    for k in range(1, 4):
        gate = gate + nn(normed[k], gate_weight[pl.ds(starts[k], 256), :])
    own_extra = as_column(extra[pl.ds(core, 1), :])
    sent = extra_other[...].astype(F32)
    other_extra = as_column(sent[0:1, 0:128] + sent[0:1, 128:256] + sent[1:2, 0:128])
    decays = -2.0 * in_lanes(rate[...]) * jax.nn.sigmoid(gate[0:256])
    decay[pl.ds(own_rows, 128), :] = decays[0:128] - own_extra
    decay[pl.ds(other_rows, 128), :] = decays[128:256] - other_extra

    for i in (1, 2):
        columns = slice(i * 256, (i + 1) * 256)
        for direction in range(2):
            kv[direction, i - 1] = convolved(padded, taps, direction, i, columns)
    going += begin([(kv, kv_out)], semaphores.at[pl.ds(3, 1)])

    log_decay = decay[...]
    inflow = minus_expm1(log_decay)
    row, col = iota((ROWS, ROWS), 0), iota((ROWS, ROWS), 1)
    same = (row // SPAN) == (col // SPAN)
    earlier = (same & (col <= row)).astype(BF16)
    later = (same & (col >= row)).astype(BF16)
    spans = (iota((ROWS, 128 * SPANS), 0) // SPAN == iota((ROWS, 128 * SPANS), 1) // 128).astype(BF16)
    for direction in range(2):
        order = later if direction else earlier
        cum[direction] = exact(lambda part, ones: nn(ones, part), log_decay, order)
        shrink[direction] = (jnp.exp(-cum[direction]) * inflow).astype(BF16)
    going += begin([(cum, cum_out), (shrink, shrink_out)], semaphores.at[pl.ds(4, 2)])
    span_totals = exact(tn, log_decay, spans)
    totals = [compact_rows(span_totals[:, n * 128 : (n + 1) * 128]) for n in range(SPANS)]
    factors = [jnp.exp(total) for total in totals]
    units = [(direction, n) for direction in range(2) for n in range(SPANS)]
    added = {}
    for direction, n in units:
        rows = slice(n * SPAN, (n + 1) * SPAN)
        local = cum[direction, rows, :]
        last = local[0:1] if direction else local[SPAN - 1 : SPAN]
        remain = (jnp.exp(last - local) * inflow[rows]).astype(BF16)
        for which in range(2):
            added[direction, n, which] = compact(tn(remain, kv[direction, which, rows, :]))
    ends = []
    for direction in range(2):
        states = [jnp.zeros((SPAN, LANES), F32), jnp.zeros((SPAN, LANES), F32)]
        passed = jnp.zeros((SPAN, LANES), F32)
        for n in reversed(range(SPANS)) if direction else range(SPANS):
            reach[direction, n] = jnp.exp(passed)
            for which in range(2):
                start[direction, n, which] = states[which].astype(BF16)
                states[which] = factors[n] * states[which] + added[direction, n, which]
            passed = passed + totals[n]
        ends.append(states)
    going += begin([(start, start_out), (reach, reach_out)], semaphores.at[pl.ds(6, 2)])
    factor = jnp.exp(totals[0] + totals[1] + totals[2] + totals[3])
    high = factor.astype(BF16).astype(F32)
    lane = iota((SPAN, LANES), 1)
    factor_parts = jnp.where(lane % 64 < 32, high, factor - high)
    for which in range(2):
        for half in range(2):
            lanes = slice(half * 128, (half + 1) * 128)
            for block in range(8):
                rows = slice(block * 8, block * 8 + 8)
                sent_out[which * 16 + half * 8 + block] = jnp.concatenate(
                    [
                        ends[0][which][rows, lanes],
                        ends[1][which][rows, lanes],
                        factor_parts[rows, lanes],
                    ],
                    axis=0,
                ).astype(BF16)
    finish(going)


def convolved(padded, taps, direction, i, columns):
    running = taps[direction, i, 0:1, :] * padded[8 : 8 + ROWS, columns]
    for j in range(1, 4):
        first = 8 + j if direction else 8 - j
        running = running + taps[direction, i, j : j + 1, :] * padded[first : first + ROWS, columns]
    return (running * jax.nn.sigmoid(running)).astype(BF16)


def own_head():
    return (iota((LANES, LANES), 0) // 64 == iota((LANES, LANES), 1) // 64).astype(BF16)


def expand(values, own):
    return jnp.concatenate([values] * 4, axis=0) * own


def seen_by(direction):
    position, other = iota((SPAN, LANES), 0), iota((SPAN, LANES), 1) % SPAN
    return other >= position if direction else other <= position


def meeting_kernel(
    query_in, kv_in, cum_in, shrink_in, start_in, taps,
    queries_out, scores_out, growth_out,
    query, keys, cum, shrink, start, padded, queries, scores, growth, semaphores,
):
    coming = begin(
        [
            (query_in, query),
            (kv_in.at[:, 0], keys),
            (cum_in, cum),
            (shrink_in, shrink),
            (start_in.at[:, :, 0], start),
        ],
        semaphores.at[pl.ds(0, 5)],
    )
    coming[0].wait()
    padded[...] = query[...].astype(F32)
    for direction in range(2):
        queries[direction] = convolved(padded, taps, direction, 0, slice(0, 256))
    going = begin([(queries, queries_out)], semaphores.at[pl.ds(5, 1)])
    finish(coming[1:])
    own = own_head()
    growth[...] = jnp.exp(cum[...])
    going += begin([(growth, growth_out)], semaphores.at[pl.ds(6, 1)])
    for n in range(SPANS):
        rows = slice(n * SPAN, (n + 1) * SPAN)
        for direction in range(2):
            asked = queries[direction, rows, :]
            meeting = nt(asked, expand(keys[direction, rows, :], own))
            meeting = jnp.where(seen_by(direction), meeting, 0.0).astype(BF16)
            scores[direction, rows, :] = growth[direction, rows, :] * (
                nn(meeting, expand(shrink[direction, rows, :], own))
                + nt(asked, expand(start[direction, n], own))
            )
    going += begin([(scores, scores_out)], semaphores.at[pl.ds(7, 1)])
    finish(going)


def scan_kernel(pieces, states_out, wide):
    count = pieces.shape[0]
    first = iota((8, 128), 1) % 64 < 32
    factors, forward, backward = [], [], []
    for i in range(count):
        piece = pieces[i].astype(F32)
        both = piece[16:24]
        factors.append(both + jnp.where(first, pltpu.roll(both, 96, 1), pltpu.roll(both, 32, 1)))
        forward.append(piece[0:8])
        backward.append(piece[8:16])
    state = jnp.zeros((8, 128), F32)
    for i in range(count):
        wide[i, 0:8, :] = state
        state = factors[i] * state + forward[i]
    state = jnp.zeros((8, 128), F32)
    for i in reversed(range(count)):
        wide[i, 8:16, :] = state
        state = factors[i] * state + backward[i]
    states_out[...] = wide[...].astype(BF16)


def head_max(values):
    first = in_first_head(values.shape[0])
    halves = []
    for half in range(2):
        part = values[:, half * 128 : (half + 1) * 128]
        left = jnp.max(jnp.where(first, part, -jnp.inf), axis=1, keepdims=True)
        right = jnp.max(jnp.where(first, -jnp.inf, part), axis=1, keepdims=True)
        halves.append(jnp.where(first, left, right))
    return jnp.concatenate(halves, axis=1)


def attention_kernel(
    own_half,
    queries_in, kv_in, shrink_in, start_in, reach_in, scores_in, growth_in, arrived, gain,
    out,
    queries, values, shrink, start, reach, scores, growth, weighted, mixing, result, entering,
    semaphores,
):
    core = lax.axis_index("core")
    half_index = core if own_half else 1 - core
    rows = pl.ds(pl.multiple_of(half_index * 128, 128), 128)
    spans = pl.ds(half_index * 2, 2)
    coming = begin(
        [
            (reach_in.at[:, spans], reach),
            (queries_in.at[:, rows, :], queries),
            (growth_in.at[:, rows, :], growth),
            (scores_in.at[:, rows, :], scores),
            (shrink_in.at[:, rows, :], shrink),
            (start_in.at[:, spans, 1], start),
            (kv_in.at[:, 1, rows, :], values),
        ],
        semaphores,
    )
    for m in range(32):
        which, half, block = m // 16, (m // 8) % 2, m % 8
        piece = arrived[m].astype(F32)
        for direction in range(2):
            entering[direction, which, block * 8 : block * 8 + 8, half * 128 : half * 128 + 128] = (
                piece[direction * 8 : direction * 8 + 8]
            )
    own = own_head()
    gains = in_lanes(gain[...])
    units = [(direction, n) for direction in range(2) for n in range(2)]
    finish(coming[:4])
    for direction, n in units:
        span = slice(n * SPAN, (n + 1) * SPAN)
        key_state = expand((reach[direction, n] * entering[direction, 0]).astype(BF16), own)
        scores[direction, span, :] = scores[direction, span, :] + growth[
            direction, span, :
        ] * nt(queries[direction, span, :], key_state)
    for direction in range(2):
        total = scores[direction]
        powers = jnp.exp(total - head_max(total))
        attend = powers / nn(powers.astype(BF16), own)
        weighted[direction] = (attend * growth[direction]).astype(BF16)
    finish(coming[4:])
    for direction, n in units:
        span = slice(n * SPAN, (n + 1) * SPAN)
        lessen = expand(shrink[direction, span, :], own)
        mixed = jnp.where(seen_by(direction), nt(weighted[direction, span, :], lessen), 0.0)
        mixing[direction, span, :] = mixed.astype(BF16)
    for direction, n in units:
        span = slice(n * SPAN, (n + 1) * SPAN)
        state = start[direction, n].astype(F32) + reach[direction, n] * entering[direction, 1]
        result[direction, span, :] = nn(
            mixing[direction, span, :], expand(values[direction, span, :], own)
        ) + nn(weighted[direction, span, :], expand(state.astype(BF16), own))
    combined = jnp.zeros((128, LANES), F32)
    for direction in range(2):
        found = result[direction]
        mean = nn((found * found).astype(BF16), own) * (1.0 / 64.0)
        combined = combined + found * lax.rsqrt(mean + EPSILON) * gains
    out[...] = combined.astype(BF16)


def tail_kernel(
    part0, part1, part2, part3, weights, tokens, gain, up, down,
    base_out, out1, out2, out3, residual, update,
):
    head = lax.axis_index("head")
    parts = (part0, part1, part2, part3)
    square = jnp.zeros((ROWS, 1), F32)
    for j in range(4):
        columns = slice(j * 256, (j + 1) * 256)
        total = nn(parts[0][...], weights[0, :, columns])
        for k in range(1, 4):
            total = total + nn(parts[k][...], weights[k, :, columns])
        value = (tokens[j].astype(F32) + total).astype(BF16).astype(F32)
        residual[j] = value
        square = square + jnp.sum(value * value, axis=1, keepdims=True)
    scale = lax.rsqrt(square * (1.0 / 1024.0) + EPSILON)
    entering = jnp.concatenate(
        [(residual[j] * scale * gain_of(gain, j)).astype(BF16) for j in range(4)], axis=1
    )
    hidden = jnp.concatenate(
        [
            jax.nn.gelu(nn(entering, up[:, j * 256 : (j + 1) * 256])).astype(BF16)
            for j in range(4)
        ],
        axis=1,
    )
    for j in range(4):
        update[j] = nn(hidden, down[:, j * 256 : (j + 1) * 256])
    base_out[...] = residual[head] + update[head]
    for k, out in ((1, out1), (2, out2), (3, out3)):
        out[...] = update[lax.rem(head + k, 4)].astype(BF16)


def finish_kernel(base, part1, part2, part3, out):
    core = lax.axis_index("core")
    total = base[...]
    for part in (part1, part2, part3):
        total = total + part[...].astype(F32)
    total = total.astype(BF16)
    out[core] = total[0:128]
    out[1 - core] = total[128:256]


def kernel(body, ins, outs, scratch=(), copies=0, flops=0):
    spaces = {"h": pltpu.HBM, "v": pltpu.VMEM}
    places = [pl.BlockSpec(memory_space=spaces[place]) for place in ins]
    shapes = [
        pltpu.HBM(out[0], out[1]) if out[2] == "h" else jax.ShapeDtypeStruct(out[0], out[1])
        for out in outs
    ]
    out_places = [pl.BlockSpec(memory_space=spaces[out[2]]) for out in outs]
    buffers = [pltpu.VMEM(shape, dtype) for shape, dtype in scratch]
    if copies:
        buffers.append(pltpu.SemaphoreType.DMA((copies,)))
    call = pl.pallas_call(
        body,
        in_specs=places,
        out_specs=out_places,
        out_shape=shapes,
        scratch_shapes=buffers,
        compiler_params=pltpu.CompilerParams(vmem_limit_bytes=32 * 1024 * 1024),
        cost_estimate=pl.CostEstimate(flops=flops, bytes_accessed=1 << 20, transcendentals=0),
    )

    def placed(*arrays):
        return call(
            *[
                pltpu.with_memory_space_constraint(array, pltpu.HBM) if place == "h" else array
                for array, place in zip(arrays, ins)
            ]
        )

    return placed


def shifted(value, k):
    count = lax.axis_size("head")
    return lax.ppermute(value, "head", [(j, (j + k) % count) for j in range(count)])


def local(
    tokens,
    input_norm_gain,
    query_key_value_weight,
    forget_gate_weight,
    convolution_filter_taps,
    slot_forget_rate,
    extra_forget_log,
    head_norm_gain,
    output_projection_weight,
    feedforward_norm_gain,
    up_projection_weight,
    down_projection_weight,
):
    chips = lax.axis_size(CHIPS)
    swap_pairs = [(0, 1), (1, 0)]
    edges, swap, mine = kernel(
        edge_kernel,
        "hh",
        [((2, 8, 256), BF16, "v"), ((136, 256), BF16, "v"), ((128, 256), BF16, "v")],
        [((2, 128, 256), BF16), ((2, 128), F32)],
        copies=2,
    )(tokens, extra_forget_log)
    ahead = [(2 * i - 1, 2 * i) for i in range(1, chips)]
    behind = [(2 * i + 2, 2 * i + 1) for i in range(chips - 1)]
    edges = lax.ppermute(edges, SEQ, ahead + behind)
    swap, kept_edge = kernel(
        swap_kernel, "vv", [((144, 256), BF16, "v"), ((8, 256), BF16, "v")]
    )(swap, edges)
    other = lax.ppermute(swap, "core", swap_pairs)
    rows = jnp.concatenate([mine, other[:128], kept_edge, other[136:]], axis=0)
    qkv_weight = jnp.transpose(query_key_value_weight, (1, 0, 2))
    rows, qkv_weight, gate_weight, out_weight = lax.optimization_barrier(
        (rows, qkv_weight, forget_gate_weight, output_projection_weight)
    )
    parts = [rows] + [shifted(rows, k) for k in (1, 2, 3)]
    qkv_weight, gate_weight, half_weight = kernel(
        warm_kernel,
        "hhh",
        [
            ((3, 1024, 256), BF16, "v"),
            ((1024, 256), BF16, "v"),
            ((128, 1024), BF16, "v"),
        ],
        copies=3,
        flops=10**9,
    )(qkv_weight, gate_weight, out_weight)
    taps = jnp.transpose(convolution_filter_taps, (0, 2, 1, 3))
    halves = (2, ROWS, LANES)
    starts = (2, SPANS, 2, SPAN, LANES)
    reaches = (2, SPANS, SPAN, LANES)
    pieces, query, kv, cum, shrink, start, reach, kept, passed = kernel(
        front_kernel,
        "v" * 11,
        [
            ((32, 24, 128), BF16, "v"),
            ((ROWS + 16, 256), BF16, "h"),
            ((2, 2, ROWS, LANES), BF16, "h"),
            (halves, F32, "h"),
            (halves, BF16, "h"),
            (starts, BF16, "h"),
            (reaches, F32, "h"),
            ((4, 128, 256), BF16, "h"),
            ((4, 128, 256), BF16, "h"),
        ],
        [
            ((ROWS + 16, 768), F32),
            ((ROWS, LANES), F32),
            ((ROWS + 16, 256), BF16),
            ((2, 2, ROWS, LANES), BF16),
            (halves, F32),
            (halves, BF16),
            (starts, BF16),
            (reaches, F32),
            ((4, 128, 256), BF16),
            ((4, 128, 256), BF16),
        ],
        copies=8,
        flops=10**9,
    )(
        *parts,
        input_norm_gain.reshape(8, 128),
        qkv_weight,
        gate_weight,
        taps,
        slot_forget_rate,
        extra_forget_log,
        other[128:136],
    )
    pieces, half_weight, passed = lax.optimization_barrier((pieces, half_weight, passed))
    held = lax.all_to_all(pieces, CHIPS, split_axis=0, concat_axis=0, tiled=True)
    own_weights, other_weights = [], []
    for k in (1, 2, 3):
        own_weights.append(shifted(half_weight, k))
        other_weights.append(lax.ppermute(own_weights[-1], "core", swap_pairs))
    passed = lax.ppermute(passed, "core", swap_pairs)
    meeting = kernel(
        meeting_kernel,
        "hhhhhv",
        [(halves, BF16, "h"), (halves, F32, "h"), (halves, F32, "h")],
        [
            ((ROWS + 16, 256), BF16),
            (halves, BF16),
            (halves, F32),
            (halves, BF16),
            (reaches, BF16),
            ((ROWS + 16, 256), F32),
            (halves, BF16),
            (halves, F32),
            (halves, F32),
        ],
        copies=8,
        flops=10**9,
    )
    queries, scores, growth = meeting(query, kv, cum, shrink, start, taps)
    (prefixes,) = kernel(
        scan_kernel, "v", [((chips, 16, 128), BF16, "v")], [((chips, 16, 128), F32)]
    )(held)
    arrived = lax.all_to_all(prefixes, CHIPS, split_axis=0, concat_axis=0, tiled=True)
    half = (2, 128, LANES)
    reached = (2, 2, SPAN, LANES)
    attention = []
    for own_half in (False, True):
        attend = kernel(
            functools.partial(attention_kernel, own_half),
            "hhhhhhhvv",
            [((128, LANES), BF16, "v")],
            [
                (half, BF16),
                (half, BF16),
                (half, BF16),
                (reached, BF16),
                (reached, F32),
                (half, F32),
                (half, F32),
                (half, BF16),
                (half, BF16),
                (half, F32),
                ((2, 2, SPAN, LANES), F32),
            ],
            copies=7,
            flops=10**9,
        )
        attention += attend(
            queries, kv, shrink, start, reach, scores, growth, arrived, head_norm_gain
        )
    swapped = lax.ppermute(attention[0], "core", swap_pairs)
    attention = jnp.concatenate([attention[1], swapped], axis=0)
    attention, down_weight = lax.optimization_barrier((attention, down_projection_weight))
    attended = [attention]
    for k in (1, 2, 3):
        attended.append(shifted(attention, k))
    warm_tail = kernel(
        warm_tail_kernel,
        "h" * 10,
        [
            ((4, 256, 1024), BF16, "v"),
            ((4, ROWS, 256), BF16, "v"),
            ((1024, 1024), BF16, "v"),
        ],
        copies=10,
        flops=10**9,
    )
    weights, whole_tokens, down_weight = warm_tail(
        output_projection_weight, *own_weights, *other_weights, kept, passed, down_weight
    )
    base, out1, out2, out3 = kernel(
        tail_kernel,
        "v" * 9,
        [((ROWS, 256), F32, "v")] + [((ROWS, 256), BF16, "v")] * 3,
        [((4, ROWS, 256), F32), ((4, ROWS, 256), F32)],
        flops=2 * 10**9,
    )(
        *attended,
        weights,
        whole_tokens,
        feedforward_norm_gain.reshape(8, 128),
        up_projection_weight,
        down_weight,
    )
    (out,) = kernel(finish_kernel, "vvvv", [((2, 128, 256), BF16, "v")])(
        base, shifted(out1, 1), shifted(out2, 2), shifted(out3, 3)
    )
    return out


def solution(mesh):
    split = Mesh(
        mesh.devices.reshape(4, 8, 2, mesh.shape["head"]), ("x", "z", "core", "head")
    )
    placed = (
        P(None, SEQ, "head"),
        P(),
        P(None, None, "head"),
        P(None, "head"),
        P(None, None, None, "head"),
        P("head", None),
        P(None, SEQ),
        P("head", None),
        P("head", None),
        P(),
        P(None, "head"),
        P("head", None),
    )

    return jax.shard_map(
        local, mesh=split, in_specs=placed, out_specs=P(None, SEQ, "head"), check_vma=False
    )
```

```python
import functools

import jax
import jax.numpy as jnp
from jax import lax
from jax.experimental import pallas as pl
from jax.experimental.pallas import tpu as pltpu
from jax.sharding import Mesh
from jax.sharding import PartitionSpec as P


CHIPS = ("x", "z")
SEQ = ("x", "z", "core")
EPSILON = 1e-06
BF16 = jnp.bfloat16
F32 = jnp.float32
SPAN = 64
ROWS = 256
LANES = 256
SPANS = ROWS // SPAN


def nn(a, b, precision=None):
    return lax.dot_general(
        a, b, (((1,), (0,)), ((), ())), preferred_element_type=F32, precision=precision
    )


def nt(a, b):
    return lax.dot_general(a, b, (((1,), (1,)), ((), ())), preferred_element_type=F32)


def tn(a, b, precision=None):
    return lax.dot_general(
        a, b, (((0,), (0,)), ((), ())), preferred_element_type=F32, precision=precision
    )


def iota(shape, dim):
    return lax.broadcasted_iota(jnp.int32, shape, dim)


def in_first_head(rows):
    return iota((rows, 128), 1) < 64


def compact(blocks):
    first = in_first_head(64)
    left = jnp.where(first, blocks[0:64, 0:128], blocks[64:128, 0:128])
    right = jnp.where(first, blocks[128:192, 128:256], blocks[192:256, 128:256])
    return jnp.concatenate([left, right], axis=1)


def compact_rows(column):
    first = in_first_head(64)
    left = jnp.where(first, column[0:64], column[64:128])
    right = jnp.where(first, column[128:192], column[192:256])
    return jnp.concatenate([left, right], axis=1)


def minus_expm1(x):
    series = 1.0 + x * (1.0 / 7.0)
    for k in (6, 5, 4, 3, 2):
        series = 1.0 + x * (1.0 / k) * series
    return jnp.where(x > -0.3, -x * series, 1.0 - jnp.exp(x))


def exact(matmul, values, zeros_and_ones):
    high = values.astype(BF16)
    rest = values - high.astype(F32)
    middle = rest.astype(BF16)
    low = (rest - middle.astype(F32)).astype(BF16)
    return (
        matmul(low, zeros_and_ones) + matmul(middle, zeros_and_ones)
    ) + matmul(high, zeros_and_ones)


def as_column(row):
    picked = jnp.where(iota((128, 128), 0) == iota((128, 128), 1), row, 0.0)
    return jnp.sum(picked, axis=1, keepdims=True)


def begin(pairs, semaphores):
    copies = [
        pltpu.make_async_copy(source, target, semaphores.at[k])
        for k, (source, target) in enumerate(pairs)
    ]
    for copy in copies:
        copy.start()
    return copies


def finish(copies):
    for copy in copies:
        copy.wait()


def in_lanes(heads):
    return jnp.concatenate([heads[h : h + 1, :] for h in range(4)], axis=1)


def gain_of(gain, source):
    return jnp.concatenate(
        [gain[pl.ds(2 * source, 1), :], gain[pl.ds(2 * source + 1, 1), :]], axis=1
    )


def warm_kernel(qkv_weight, gate_weight, out_weight, qkv_out, gate_out, half_out, semaphores):
    rows = pl.ds(pl.multiple_of(lax.axis_index("core") * 128, 128), 128)
    finish(
        begin(
            [
                (qkv_weight, qkv_out),
                (gate_weight, gate_out),
                (out_weight.at[rows, :], half_out),
            ],
            semaphores,
        )
    )


def warm_tail_kernel(
    weight0, mine1, mine2, mine3, theirs1, theirs2, theirs3, kept, passed, down,
    weights_out, tokens_out, down_out, semaphores,
):
    core = lax.axis_index("core")
    own = pl.ds(pl.multiple_of(core * 128, 128), 128)
    other = pl.ds(pl.multiple_of((1 - core) * 128, 128), 128)
    pairs = [(weight0, weights_out.at[0])]
    for k, mine, theirs in ((1, mine1, theirs1), (2, mine2, theirs2), (3, mine3, theirs3)):
        pairs += [(mine, weights_out.at[k, own]), (theirs, weights_out.at[k, other])]
    pairs += [(kept, tokens_out.at[:, 0:128]), (passed, tokens_out.at[:, 128:256])]
    finish(begin(pairs + [(down, down_out)], semaphores))


def edge_kernel(tokens_in, extra_in, edge_out, swap_out, mine_out, tokens, extra, semaphores):
    core = lax.axis_index("core")
    finish(begin([(tokens_in, tokens), (extra_in, extra)], semaphores))
    mine_out[...] = tokens[core]
    for which in range(2):
        wide = tokens[which].astype(F32)
        edge_out[which] = jnp.where(core == 1, wide[120:128], wide[0:8]).astype(BF16)
    row = extra[pl.ds(1 - core, 1), :]
    high = row.astype(BF16).astype(F32)
    middle = (row - high).astype(BF16).astype(F32)
    low = row - high - middle
    line = iota((8, 256), 0)
    first = jnp.concatenate([high, middle], axis=1)
    second = jnp.concatenate([low, low], axis=1)
    packed = jnp.where(line == 0, first, jnp.where(line == 1, second, 0.0))
    swap_out[0:128] = tokens[1 - core]
    swap_out[128:136] = packed.astype(BF16)


def swap_kernel(local_part, edges, swap_out, kept_out):
    core = lax.axis_index("core")
    swap_out[0:136] = local_part[...]
    swap_out[136:144] = edges[1 - core]
    kept_out[...] = edges[core]


def front_kernel(
    part0, part1, part2, part3, gain, qkv_weight, gate_weight, taps, rate, extra, extra_other,
    sent_out, query_out, kv_out, cum_out, shrink_out, start_out, reach_out, kept_out, passed_out,
    padded, decay, query, kv, cum, shrink, start, reach, kept, passed_on, semaphores,
):
    core = lax.axis_index("core")
    head = lax.axis_index("head")
    parts = (part0, part1, part2, part3)
    sources = [lax.rem(head + 4 - k, 4) for k in range(4)]
    own_rows = pl.multiple_of(core * 128, 128)
    other_rows = pl.multiple_of((1 - core) * 128, 128)
    square = jnp.zeros((ROWS + 16, 1), F32)
    for k in range(4):
        values = parts[k][...]
        kept[sources[k]] = values[0:128]
        passed_on[sources[k]] = values[128:256]
        wide = values.astype(F32)
        square = square + jnp.sum(wide * wide, axis=1, keepdims=True)
    going = begin([(kept, kept_out), (passed_on, passed_out)], semaphores.at[pl.ds(0, 2)])
    scale = lax.rsqrt(square * (1.0 / 1024.0) + EPSILON)
    normed = [
        (parts[k][...].astype(F32) * scale * gain_of(gain, sources[k])).astype(BF16)
        for k in range(4)
    ]
    starts = [pl.multiple_of(source * 256, 256) for source in sources]
    own_pad = pl.multiple_of(8 + core * 128, 8)
    other_pad = pl.multiple_of(8 + (1 - core) * 128, 8)
    a_pad = pl.multiple_of(core * 264, 8)
    b_pad = pl.multiple_of((1 - core) * 264, 8)
    for i in range(3):
        total = nn(normed[0], qkv_weight[i, pl.ds(starts[0], 256), :])
        for k in range(1, 4):
            total = total + nn(normed[k], qkv_weight[i, pl.ds(starts[k], 256), :])
        total = total.astype(BF16).astype(F32)
        columns = slice(i * 256, (i + 1) * 256)
        padded[pl.ds(own_pad, 128), columns] = total[0:128]
        padded[pl.ds(other_pad, 128), columns] = total[128:256]
        padded[pl.ds(a_pad, 8), columns] = total[256:264]
        padded[pl.ds(b_pad, 8), columns] = total[264:272]
    query[...] = padded[:, 0:256].astype(BF16)
    going += begin([(query, query_out)], semaphores.at[pl.ds(2, 1)])
    gate = nn(normed[0], gate_weight[pl.ds(starts[0], 256), :])
    for k in range(1, 4):
        gate = gate + nn(normed[k], gate_weight[pl.ds(starts[k], 256), :])
    own_extra = as_column(extra[pl.ds(core, 1), :])
    sent = extra_other[...].astype(F32)
    other_extra = as_column(sent[0:1, 0:128] + sent[0:1, 128:256] + sent[1:2, 0:128])
    decays = -2.0 * in_lanes(rate[...]) * jax.nn.sigmoid(gate[0:256])
    decay[pl.ds(own_rows, 128), :] = decays[0:128] - own_extra
    decay[pl.ds(other_rows, 128), :] = decays[128:256] - other_extra

    for i in (1, 2):
        columns = slice(i * 256, (i + 1) * 256)
        for direction in range(2):
            kv[direction, i - 1] = convolved(padded, taps, direction, i, columns)
    going += begin([(kv, kv_out)], semaphores.at[pl.ds(3, 1)])

    log_decay = decay[...]
    inflow = minus_expm1(log_decay)
    row, col = iota((ROWS, ROWS), 0), iota((ROWS, ROWS), 1)
    same = (row // SPAN) == (col // SPAN)
    earlier = (same & (col <= row)).astype(BF16)
    later = (same & (col >= row)).astype(BF16)
    spans = (iota((ROWS, 128 * SPANS), 0) // SPAN == iota((ROWS, 128 * SPANS), 1) // 128).astype(BF16)
    for direction in range(2):
        order = later if direction else earlier
        cum[direction] = exact(lambda part, ones: nn(ones, part), log_decay, order)
        shrink[direction] = (jnp.exp(-cum[direction]) * inflow).astype(BF16)
    going += begin([(cum, cum_out), (shrink, shrink_out)], semaphores.at[pl.ds(4, 2)])
    span_totals = exact(tn, log_decay, spans)
    totals = [compact_rows(span_totals[:, n * 128 : (n + 1) * 128]) for n in range(SPANS)]
    factors = [jnp.exp(total) for total in totals]
    units = [(direction, n) for direction in range(2) for n in range(SPANS)]
    added = {}
    for direction, n in units:
        rows = slice(n * SPAN, (n + 1) * SPAN)
        local = cum[direction, rows, :]
        last = local[0:1] if direction else local[SPAN - 1 : SPAN]
        remain = (jnp.exp(last - local) * inflow[rows]).astype(BF16)
        for which in range(2):
            added[direction, n, which] = compact(tn(remain, kv[direction, which, rows, :]))
    ends = []
    for direction in range(2):
        states = [jnp.zeros((SPAN, LANES), F32), jnp.zeros((SPAN, LANES), F32)]
        passed = jnp.zeros((SPAN, LANES), F32)
        for n in reversed(range(SPANS)) if direction else range(SPANS):
            reach[direction, n] = jnp.exp(passed)
            for which in range(2):
                start[direction, n, which] = states[which].astype(BF16)
                states[which] = factors[n] * states[which] + added[direction, n, which]
            passed = passed + totals[n]
        ends.append(states)
    going += begin([(start, start_out), (reach, reach_out)], semaphores.at[pl.ds(6, 2)])
    factor = jnp.exp(totals[0] + totals[1] + totals[2] + totals[3])
    high = factor.astype(BF16).astype(F32)
    lane = iota((SPAN, LANES), 1)
    factor_parts = jnp.where(lane % 64 < 32, high, factor - high)
    for which in range(2):
        for half in range(2):
            lanes = slice(half * 128, (half + 1) * 128)
            for block in range(8):
                rows = slice(block * 8, block * 8 + 8)
                sent_out[which * 16 + half * 8 + block] = jnp.concatenate(
                    [
                        ends[0][which][rows, lanes],
                        ends[1][which][rows, lanes],
                        factor_parts[rows, lanes],
                    ],
                    axis=0,
                ).astype(BF16)
    finish(going)


def convolved(padded, taps, direction, i, columns):
    running = taps[direction, i, 0:1, :] * padded[8 : 8 + ROWS, columns]
    for j in range(1, 4):
        first = 8 + j if direction else 8 - j
        running = running + taps[direction, i, j : j + 1, :] * padded[first : first + ROWS, columns]
    return (running * jax.nn.sigmoid(running)).astype(BF16)


def own_head():
    return (iota((LANES, LANES), 0) // 64 == iota((LANES, LANES), 1) // 64).astype(BF16)


def expand(values, own):
    return jnp.concatenate([values] * 4, axis=0) * own


def seen_by(direction):
    position, other = iota((SPAN, LANES), 0), iota((SPAN, LANES), 1) % SPAN
    return other >= position if direction else other <= position


def meeting_kernel(
    query_in, kv_in, cum_in, shrink_in, start_in, taps,
    queries_out, scores_out, growth_out,
    query, keys, cum, shrink, start, padded, queries, scores, growth, semaphores,
):
    coming = begin(
        [
            (query_in, query),
            (kv_in.at[:, 0], keys),
            (cum_in, cum),
            (shrink_in, shrink),
            (start_in.at[:, :, 0], start),
        ],
        semaphores.at[pl.ds(0, 5)],
    )
    coming[0].wait()
    padded[...] = query[...].astype(F32)
    for direction in range(2):
        queries[direction] = convolved(padded, taps, direction, 0, slice(0, 256))
    going = begin([(queries, queries_out)], semaphores.at[pl.ds(5, 1)])
    finish(coming[1:])
    own = own_head()
    growth[...] = jnp.exp(cum[...])
    going += begin([(growth, growth_out)], semaphores.at[pl.ds(6, 1)])
    for n in range(SPANS):
        rows = slice(n * SPAN, (n + 1) * SPAN)
        for direction in range(2):
            asked = queries[direction, rows, :]
            meeting = nt(asked, expand(keys[direction, rows, :], own))
            meeting = jnp.where(seen_by(direction), meeting, 0.0).astype(BF16)
            scores[direction, rows, :] = growth[direction, rows, :] * (
                nn(meeting, expand(shrink[direction, rows, :], own))
                + nt(asked, expand(start[direction, n], own))
            )
    going += begin([(scores, scores_out)], semaphores.at[pl.ds(7, 1)])
    finish(going)


def scan_kernel(pieces, states_out, wide):
    count = pieces.shape[0]
    first = iota((8, 128), 1) % 64 < 32
    factors, forward, backward = [], [], []
    for i in range(count):
        piece = pieces[i].astype(F32)
        both = piece[16:24]
        factors.append(both + jnp.where(first, pltpu.roll(both, 96, 1), pltpu.roll(both, 32, 1)))
        forward.append(piece[0:8])
        backward.append(piece[8:16])
    state = jnp.zeros((8, 128), F32)
    for i in range(count):
        wide[i, 0:8, :] = state
        state = factors[i] * state + forward[i]
    state = jnp.zeros((8, 128), F32)
    for i in reversed(range(count)):
        wide[i, 8:16, :] = state
        state = factors[i] * state + backward[i]
    states_out[...] = wide[...].astype(BF16)


def head_max(values):
    first = in_first_head(values.shape[0])
    halves = []
    for half in range(2):
        part = values[:, half * 128 : (half + 1) * 128]
        left = jnp.max(jnp.where(first, part, -jnp.inf), axis=1, keepdims=True)
        right = jnp.max(jnp.where(first, -jnp.inf, part), axis=1, keepdims=True)
        halves.append(jnp.where(first, left, right))
    return jnp.concatenate(halves, axis=1)


def attention_kernel(
    own_half,
    queries_in, kv_in, shrink_in, start_in, reach_in, scores_in, growth_in, arrived, gain,
    out,
    queries, values, shrink, start, reach, scores, growth, weighted, mixing, result, entering,
    semaphores,
):
    core = lax.axis_index("core")
    half_index = core if own_half else 1 - core
    rows = pl.ds(pl.multiple_of(half_index * 128, 128), 128)
    spans = pl.ds(half_index * 2, 2)
    coming = begin(
        [
            (reach_in.at[:, spans], reach),
            (queries_in.at[:, rows, :], queries),
            (growth_in.at[:, rows, :], growth),
            (scores_in.at[:, rows, :], scores),
            (shrink_in.at[:, rows, :], shrink),
            (start_in.at[:, spans, 1], start),
            (kv_in.at[:, 1, rows, :], values),
        ],
        semaphores,
    )
    for m in range(32):
        which, half, block = m // 16, (m // 8) % 2, m % 8
        piece = arrived[m].astype(F32)
        for direction in range(2):
            entering[direction, which, block * 8 : block * 8 + 8, half * 128 : half * 128 + 128] = (
                piece[direction * 8 : direction * 8 + 8]
            )
    own = own_head()
    gains = in_lanes(gain[...])
    units = [(direction, n) for direction in range(2) for n in range(2)]
    finish(coming[:4])
    for direction, n in units:
        span = slice(n * SPAN, (n + 1) * SPAN)
        key_state = expand((reach[direction, n] * entering[direction, 0]).astype(BF16), own)
        scores[direction, span, :] = scores[direction, span, :] + growth[
            direction, span, :
        ] * nt(queries[direction, span, :], key_state)
    for direction in range(2):
        total = scores[direction]
        powers = jnp.exp(total - head_max(total))
        attend = powers / nn(powers.astype(BF16), own)
        weighted[direction] = (attend * growth[direction]).astype(BF16)
    finish(coming[4:])
    for direction, n in units:
        span = slice(n * SPAN, (n + 1) * SPAN)
        lessen = expand(shrink[direction, span, :], own)
        mixed = jnp.where(seen_by(direction), nt(weighted[direction, span, :], lessen), 0.0)
        mixing[direction, span, :] = mixed.astype(BF16)
    for direction, n in units:
        span = slice(n * SPAN, (n + 1) * SPAN)
        state = start[direction, n].astype(F32) + reach[direction, n] * entering[direction, 1]
        result[direction, span, :] = nn(
            mixing[direction, span, :], expand(values[direction, span, :], own)
        ) + nn(weighted[direction, span, :], expand(state.astype(BF16), own))
    combined = jnp.zeros((128, LANES), F32)
    for direction in range(2):
        found = result[direction]
        mean = nn((found * found).astype(BF16), own) * (1.0 / 64.0)
        combined = combined + found * lax.rsqrt(mean + EPSILON) * gains
    out[...] = combined.astype(BF16)


def tail_kernel(
    part0, part1, part2, part3, weights, tokens, gain, up, down,
    base_out, out1, out2, out3, residual, update,
):
    head = lax.axis_index("head")
    parts = (part0, part1, part2, part3)
    square = jnp.zeros((ROWS, 1), F32)
    for j in range(4):
        columns = slice(j * 256, (j + 1) * 256)
        total = nn(parts[0][...], weights[0, :, columns])
        for k in range(1, 4):
            total = total + nn(parts[k][...], weights[k, :, columns])
        value = (tokens[j].astype(F32) + total).astype(BF16).astype(F32)
        residual[j] = value
        square = square + jnp.sum(value * value, axis=1, keepdims=True)
    scale = lax.rsqrt(square * (1.0 / 1024.0) + EPSILON)
    entering = jnp.concatenate(
        [(residual[j] * scale * gain_of(gain, j)).astype(BF16) for j in range(4)], axis=1
    )
    hidden = jnp.concatenate(
        [
            jax.nn.gelu(nn(entering, up[:, j * 256 : (j + 1) * 256])).astype(BF16)
            for j in range(4)
        ],
        axis=1,
    )
    for j in range(4):
        update[j] = nn(hidden, down[:, j * 256 : (j + 1) * 256])
    base_out[...] = residual[head] + update[head]
    for k, out in ((1, out1), (2, out2), (3, out3)):
        out[...] = update[lax.rem(head + k, 4)].astype(BF16)


def finish_kernel(base, part1, part2, part3, out):
    core = lax.axis_index("core")
    total = base[...]
    for part in (part1, part2, part3):
        total = total + part[...].astype(F32)
    total = total.astype(BF16)
    out[core] = total[0:128]
    out[1 - core] = total[128:256]


def kernel(body, ins, outs, scratch=(), copies=0, flops=0):
    spaces = {"h": pltpu.HBM, "v": pltpu.VMEM}
    places = [pl.BlockSpec(memory_space=spaces[place]) for place in ins]
    shapes = [
        pltpu.HBM(out[0], out[1]) if out[2] == "h" else jax.ShapeDtypeStruct(out[0], out[1])
        for out in outs
    ]
    out_places = [pl.BlockSpec(memory_space=spaces[out[2]]) for out in outs]
    buffers = [pltpu.VMEM(shape, dtype) for shape, dtype in scratch]
    if copies:
        buffers.append(pltpu.SemaphoreType.DMA((copies,)))
    call = pl.pallas_call(
        body,
        in_specs=places,
        out_specs=out_places,
        out_shape=shapes,
        scratch_shapes=buffers,
        compiler_params=pltpu.CompilerParams(vmem_limit_bytes=32 * 1024 * 1024),
        cost_estimate=pl.CostEstimate(flops=flops, bytes_accessed=1 << 20, transcendentals=0),
    )

    def placed(*arrays):
        return call(
            *[
                pltpu.with_memory_space_constraint(array, pltpu.HBM) if place == "h" else array
                for array, place in zip(arrays, ins)
            ]
        )

    return placed


def shifted(value, k):
    count = lax.axis_size("head")
    return lax.ppermute(value, "head", [(j, (j + k) % count) for j in range(count)])


def local(
    tokens,
    input_norm_gain,
    query_key_value_weight,
    forget_gate_weight,
    convolution_filter_taps,
    slot_forget_rate,
    extra_forget_log,
    head_norm_gain,
    output_projection_weight,
    feedforward_norm_gain,
    up_projection_weight,
    down_projection_weight,
):
    chips = lax.axis_size(CHIPS)
    swap_pairs = [(0, 1), (1, 0)]
    edges, swap, mine = kernel(
        edge_kernel,
        "hh",
        [((2, 8, 256), BF16, "v"), ((136, 256), BF16, "v"), ((128, 256), BF16, "v")],
        [((2, 128, 256), BF16), ((2, 128), F32)],
        copies=2,
    )(tokens, extra_forget_log)
    ahead = [(2 * i - 1, 2 * i) for i in range(1, chips)]
    behind = [(2 * i + 2, 2 * i + 1) for i in range(chips - 1)]
    edges = lax.ppermute(edges, SEQ, ahead + behind)
    swap, kept_edge = kernel(
        swap_kernel, "vv", [((144, 256), BF16, "v"), ((8, 256), BF16, "v")]
    )(swap, edges)
    other = lax.ppermute(swap, "core", swap_pairs)
    rows = jnp.concatenate([mine, other[:128], kept_edge, other[136:]], axis=0)
    qkv_weight = jnp.transpose(query_key_value_weight, (1, 0, 2))
    rows, qkv_weight, gate_weight, out_weight = lax.optimization_barrier(
        (rows, qkv_weight, forget_gate_weight, output_projection_weight)
    )
    parts = [rows]
    for k in (1, 2, 3):
        parts.append(shifted(rows, k))
    qkv_weight, gate_weight, half_weight = kernel(
        warm_kernel,
        "hhh",
        [
            ((3, 1024, 256), BF16, "v"),
            ((1024, 256), BF16, "v"),
            ((128, 1024), BF16, "v"),
        ],
        copies=3,
        flops=10**9,
    )(qkv_weight, gate_weight, out_weight)
    taps = jnp.transpose(convolution_filter_taps, (0, 2, 1, 3))
    halves = (2, ROWS, LANES)
    starts = (2, SPANS, 2, SPAN, LANES)
    reaches = (2, SPANS, SPAN, LANES)
    pieces, query, kv, cum, shrink, start, reach, kept, passed = kernel(
        front_kernel,
        "v" * 11,
        [
            ((32, 24, 128), BF16, "v"),
            ((ROWS + 16, 256), BF16, "h"),
            ((2, 2, ROWS, LANES), BF16, "h"),
            (halves, F32, "h"),
            (halves, BF16, "h"),
            (starts, BF16, "h"),
            (reaches, F32, "h"),
            ((4, 128, 256), BF16, "h"),
            ((4, 128, 256), BF16, "h"),
        ],
        [
            ((ROWS + 16, 768), F32),
            ((ROWS, LANES), F32),
            ((ROWS + 16, 256), BF16),
            ((2, 2, ROWS, LANES), BF16),
            (halves, F32),
            (halves, BF16),
            (starts, BF16),
            (reaches, F32),
            ((4, 128, 256), BF16),
            ((4, 128, 256), BF16),
        ],
        copies=8,
        flops=10**9,
    )(
        *parts,
        input_norm_gain.reshape(8, 128),
        qkv_weight,
        gate_weight,
        taps,
        slot_forget_rate,
        extra_forget_log,
        other[128:136],
    )
    pieces, half_weight, passed = lax.optimization_barrier((pieces, half_weight, passed))
    held = lax.all_to_all(pieces, CHIPS, split_axis=0, concat_axis=0, tiled=True)
    own_weights, other_weights = [], []
    for k in (1, 2, 3):
        own_weights.append(shifted(half_weight, k))
        other_weights.append(lax.ppermute(own_weights[-1], "core", swap_pairs))
    passed = lax.ppermute(passed, "core", swap_pairs)
    meeting = kernel(
        meeting_kernel,
        "hhhhhv",
        [(halves, BF16, "h"), (halves, F32, "h"), (halves, F32, "h")],
        [
            ((ROWS + 16, 256), BF16),
            (halves, BF16),
            (halves, F32),
            (halves, BF16),
            (reaches, BF16),
            ((ROWS + 16, 256), F32),
            (halves, BF16),
            (halves, F32),
            (halves, F32),
        ],
        copies=8,
        flops=10**9,
    )
    queries, scores, growth = meeting(query, kv, cum, shrink, start, taps)
    (prefixes,) = kernel(
        scan_kernel, "v", [((chips, 16, 128), BF16, "v")], [((chips, 16, 128), F32)]
    )(held)
    arrived = lax.all_to_all(prefixes, CHIPS, split_axis=0, concat_axis=0, tiled=True)
    half = (2, 128, LANES)
    reached = (2, 2, SPAN, LANES)
    attention = []
    for own_half in (False, True):
        attend = kernel(
            functools.partial(attention_kernel, own_half),
            "hhhhhhhvv",
            [((128, LANES), BF16, "v")],
            [
                (half, BF16),
                (half, BF16),
                (half, BF16),
                (reached, BF16),
                (reached, F32),
                (half, F32),
                (half, F32),
                (half, BF16),
                (half, BF16),
                (half, F32),
                ((2, 2, SPAN, LANES), F32),
            ],
            copies=7,
            flops=10**9,
        )
        attention += attend(
            queries, kv, shrink, start, reach, scores, growth, arrived, head_norm_gain
        )
    swapped = lax.ppermute(attention[0], "core", swap_pairs)
    attention = jnp.concatenate([attention[1], swapped], axis=0)
    attention, down_weight = lax.optimization_barrier((attention, down_projection_weight))
    attended = [attention]
    for k in (1, 2, 3):
        attended.append(shifted(attention, k))
    warm_tail = kernel(
        warm_tail_kernel,
        "h" * 10,
        [
            ((4, 256, 1024), BF16, "v"),
            ((4, ROWS, 256), BF16, "v"),
            ((1024, 1024), BF16, "v"),
        ],
        copies=10,
        flops=10**9,
    )
    weights, whole_tokens, down_weight = warm_tail(
        output_projection_weight, *own_weights, *other_weights, kept, passed, down_weight
    )
    base, out1, out2, out3 = kernel(
        tail_kernel,
        "v" * 9,
        [((ROWS, 256), F32, "v")] + [((ROWS, 256), BF16, "v")] * 3,
        [((4, ROWS, 256), F32), ((4, ROWS, 256), F32)],
        flops=2 * 10**9,
    )(
        *attended,
        weights,
        whole_tokens,
        feedforward_norm_gain.reshape(8, 128),
        up_projection_weight,
        down_weight,
    )
    sums = [base]
    for k, part in ((1, out1), (2, out2), (3, out3)):
        sums.append(shifted(part, k))
    (out,) = kernel(finish_kernel, "vvvv", [((2, 128, 256), BF16, "v")])(*sums)
    return out


def solution(mesh):
    split = Mesh(
        mesh.devices.reshape(4, 8, 2, mesh.shape["head"]), ("x", "z", "core", "head")
    )
    placed = (
        P(None, SEQ, "head"),
        P(),
        P(None, None, "head"),
        P(None, "head"),
        P(None, None, None, "head"),
        P("head", None),
        P(None, SEQ),
        P("head", None),
        P("head", None),
        P(),
        P(None, "head"),
        P("head", None),
    )

    return jax.shard_map(
        local, mesh=split, in_specs=placed, out_specs=P(None, SEQ, "head"), check_vma=False
    )
```

```python
import functools

import jax
import jax.numpy as jnp
from jax import lax
from jax.experimental import pallas as pl
from jax.experimental.pallas import tpu as pltpu
from jax.sharding import Mesh
from jax.sharding import PartitionSpec as P


CHIPS = ("x", "z")
SEQ = ("x", "z", "core")
EPSILON = 1e-06
BF16 = jnp.bfloat16
F32 = jnp.float32
SPAN = 64
ROWS = 256
LANES = 256
SPANS = ROWS // SPAN


def nn(a, b, precision=None):
    return lax.dot_general(
        a, b, (((1,), (0,)), ((), ())), preferred_element_type=F32, precision=precision
    )


def nt(a, b):
    return lax.dot_general(a, b, (((1,), (1,)), ((), ())), preferred_element_type=F32)


def tn(a, b, precision=None):
    return lax.dot_general(
        a, b, (((0,), (0,)), ((), ())), preferred_element_type=F32, precision=precision
    )


def iota(shape, dim):
    return lax.broadcasted_iota(jnp.int32, shape, dim)


def in_first_head(rows):
    return iota((rows, 128), 1) < 64


def compact(blocks):
    first = in_first_head(64)
    left = jnp.where(first, blocks[0:64, 0:128], blocks[64:128, 0:128])
    right = jnp.where(first, blocks[128:192, 128:256], blocks[192:256, 128:256])
    return jnp.concatenate([left, right], axis=1)


def compact_rows(column):
    first = in_first_head(64)
    left = jnp.where(first, column[0:64], column[64:128])
    right = jnp.where(first, column[128:192], column[192:256])
    return jnp.concatenate([left, right], axis=1)


def minus_expm1(x):
    series = 1.0 + x * (1.0 / 7.0)
    for k in (6, 5, 4, 3, 2):
        series = 1.0 + x * (1.0 / k) * series
    return jnp.where(x > -0.3, -x * series, 1.0 - jnp.exp(x))


def exact(matmul, values, zeros_and_ones):
    high = values.astype(BF16)
    rest = values - high.astype(F32)
    middle = rest.astype(BF16)
    low = (rest - middle.astype(F32)).astype(BF16)
    return (
        matmul(low, zeros_and_ones) + matmul(middle, zeros_and_ones)
    ) + matmul(high, zeros_and_ones)


def as_column(row):
    picked = jnp.where(iota((128, 128), 0) == iota((128, 128), 1), row, 0.0)
    return jnp.sum(picked, axis=1, keepdims=True)


def begin(pairs, semaphores):
    copies = [
        pltpu.make_async_copy(source, target, semaphores.at[k])
        for k, (source, target) in enumerate(pairs)
    ]
    for copy in copies:
        copy.start()
    return copies


def finish(copies):
    for copy in copies:
        copy.wait()


def in_lanes(heads):
    return jnp.concatenate([heads[h : h + 1, :] for h in range(4)], axis=1)


def gain_of(gain, source):
    return jnp.concatenate(
        [gain[pl.ds(2 * source, 1), :], gain[pl.ds(2 * source + 1, 1), :]], axis=1
    )


def warm_kernel(qkv_weight, gate_weight, out_weight, qkv_out, gate_out, half_out, semaphores):
    rows = pl.ds(pl.multiple_of(lax.axis_index("core") * 128, 128), 128)
    finish(
        begin(
            [
                (qkv_weight, qkv_out),
                (gate_weight, gate_out),
                (out_weight.at[rows, :], half_out),
            ],
            semaphores,
        )
    )


def warm_tail_kernel(
    weight0, mine1, mine2, mine3, theirs1, theirs2, theirs3, kept, passed, down,
    weights_out, tokens_out, down_out, semaphores,
):
    core = lax.axis_index("core")
    own = pl.ds(pl.multiple_of(core * 128, 128), 128)
    other = pl.ds(pl.multiple_of((1 - core) * 128, 128), 128)
    pairs = [(weight0, weights_out.at[0])]
    for k, mine, theirs in ((1, mine1, theirs1), (2, mine2, theirs2), (3, mine3, theirs3)):
        pairs += [(mine, weights_out.at[k, own]), (theirs, weights_out.at[k, other])]
    pairs += [(kept, tokens_out.at[:, 0:128]), (passed, tokens_out.at[:, 128:256])]
    finish(begin(pairs + [(down, down_out)], semaphores))


def edge_kernel(tokens_in, extra_in, edge_out, swap_out, mine_out, tokens, extra, semaphores):
    core = lax.axis_index("core")
    finish(begin([(tokens_in, tokens), (extra_in, extra)], semaphores))
    mine_out[...] = tokens[core]
    for which in range(2):
        wide = tokens[which].astype(F32)
        edge_out[which] = jnp.where(core == 1, wide[120:128], wide[0:8]).astype(BF16)
    row = extra[pl.ds(1 - core, 1), :]
    high = row.astype(BF16).astype(F32)
    middle = (row - high).astype(BF16).astype(F32)
    low = row - high - middle
    line = iota((8, 256), 0)
    first = jnp.concatenate([high, middle], axis=1)
    second = jnp.concatenate([low, low], axis=1)
    packed = jnp.where(line == 0, first, jnp.where(line == 1, second, 0.0))
    swap_out[0:128] = tokens[1 - core]
    swap_out[128:136] = packed.astype(BF16)


def pick_kernel(edges, sent_out, kept_out):
    core = lax.axis_index("core")
    sent_out[...] = edges[1 - core]
    kept_out[...] = edges[core]


def front_kernel(
    part0, part1, part2, part3, halo0, halo1, halo2, halo3, gain, qkv_weight, gate_weight, taps, rate, extra, extra_other,
    sent_out, query_out, kv_out, cum_out, shrink_out, start_out, reach_out, kept_out, passed_out,
    padded, decay, query, kv, cum, shrink, start, reach, kept, passed_on, semaphores,
):
    core = lax.axis_index("core")
    head = lax.axis_index("head")
    parts = (part0, part1, part2, part3)
    halos = (halo0, halo1, halo2, halo3)
    sources = [lax.rem(head + 4 - k, 4) for k in range(4)]
    own_rows = pl.multiple_of(core * 128, 128)
    other_rows = pl.multiple_of((1 - core) * 128, 128)
    square = jnp.zeros((ROWS + 16, 1), F32)
    for k in range(4):
        kept[sources[k]] = parts[k][0:128]
        passed_on[sources[k]] = parts[k][128:256]
        wide = jnp.concatenate([parts[k][...], halos[k][...]], axis=0).astype(F32)
        square = square + jnp.sum(wide * wide, axis=1, keepdims=True)
    going = begin([(kept, kept_out), (passed_on, passed_out)], semaphores.at[pl.ds(0, 2)])
    scale = lax.rsqrt(square * (1.0 / 1024.0) + EPSILON)
    normed = [
        (
            jnp.concatenate([parts[k][...], halos[k][...]], axis=0).astype(F32)
            * scale
            * gain_of(gain, sources[k])
        ).astype(BF16)
        for k in range(4)
    ]
    starts = [pl.multiple_of(source * 256, 256) for source in sources]
    own_pad = pl.multiple_of(8 + core * 128, 8)
    other_pad = pl.multiple_of(8 + (1 - core) * 128, 8)
    a_pad = pl.multiple_of(core * 264, 8)
    b_pad = pl.multiple_of((1 - core) * 264, 8)
    for i in range(3):
        total = nn(normed[0], qkv_weight[i, pl.ds(starts[0], 256), :])
        for k in range(1, 4):
            total = total + nn(normed[k], qkv_weight[i, pl.ds(starts[k], 256), :])
        total = total.astype(BF16).astype(F32)
        columns = slice(i * 256, (i + 1) * 256)
        padded[pl.ds(own_pad, 128), columns] = total[0:128]
        padded[pl.ds(other_pad, 128), columns] = total[128:256]
        padded[pl.ds(a_pad, 8), columns] = total[256:264]
        padded[pl.ds(b_pad, 8), columns] = total[264:272]
    query[...] = padded[:, 0:256].astype(BF16)
    going += begin([(query, query_out)], semaphores.at[pl.ds(2, 1)])
    gate = nn(normed[0], gate_weight[pl.ds(starts[0], 256), :])
    for k in range(1, 4):
        gate = gate + nn(normed[k], gate_weight[pl.ds(starts[k], 256), :])
    own_extra = as_column(extra[pl.ds(core, 1), :])
    sent = extra_other[...].astype(F32)
    other_extra = as_column(sent[0:1, 0:128] + sent[0:1, 128:256] + sent[1:2, 0:128])
    decays = -2.0 * in_lanes(rate[...]) * jax.nn.sigmoid(gate[0:256])
    decay[pl.ds(own_rows, 128), :] = decays[0:128] - own_extra
    decay[pl.ds(other_rows, 128), :] = decays[128:256] - other_extra

    for i in (1, 2):
        columns = slice(i * 256, (i + 1) * 256)
        for direction in range(2):
            kv[direction, i - 1] = convolved(padded, taps, direction, i, columns)
    going += begin([(kv, kv_out)], semaphores.at[pl.ds(3, 1)])

    log_decay = decay[...]
    inflow = minus_expm1(log_decay)
    row, col = iota((ROWS, ROWS), 0), iota((ROWS, ROWS), 1)
    same = (row // SPAN) == (col // SPAN)
    earlier = (same & (col <= row)).astype(BF16)
    later = (same & (col >= row)).astype(BF16)
    spans = (iota((ROWS, 128 * SPANS), 0) // SPAN == iota((ROWS, 128 * SPANS), 1) // 128).astype(BF16)
    for direction in range(2):
        order = later if direction else earlier
        cum[direction] = exact(lambda part, ones: nn(ones, part), log_decay, order)
        shrink[direction] = (jnp.exp(-cum[direction]) * inflow).astype(BF16)
    going += begin([(cum, cum_out), (shrink, shrink_out)], semaphores.at[pl.ds(4, 2)])
    span_totals = exact(tn, log_decay, spans)
    totals = [compact_rows(span_totals[:, n * 128 : (n + 1) * 128]) for n in range(SPANS)]
    factors = [jnp.exp(total) for total in totals]
    units = [(direction, n) for direction in range(2) for n in range(SPANS)]
    added = {}
    for direction, n in units:
        rows = slice(n * SPAN, (n + 1) * SPAN)
        local = cum[direction, rows, :]
        last = local[0:1] if direction else local[SPAN - 1 : SPAN]
        remain = (jnp.exp(last - local) * inflow[rows]).astype(BF16)
        for which in range(2):
            added[direction, n, which] = compact(tn(remain, kv[direction, which, rows, :]))
    ends = []
    for direction in range(2):
        states = [jnp.zeros((SPAN, LANES), F32), jnp.zeros((SPAN, LANES), F32)]
        passed = jnp.zeros((SPAN, LANES), F32)
        for n in reversed(range(SPANS)) if direction else range(SPANS):
            reach[direction, n] = jnp.exp(passed)
            for which in range(2):
                start[direction, n, which] = states[which].astype(BF16)
                states[which] = factors[n] * states[which] + added[direction, n, which]
            passed = passed + totals[n]
        ends.append(states)
    going += begin([(start, start_out), (reach, reach_out)], semaphores.at[pl.ds(6, 2)])
    factor = jnp.exp(totals[0] + totals[1] + totals[2] + totals[3])
    high = factor.astype(BF16).astype(F32)
    lane = iota((SPAN, LANES), 1)
    factor_parts = jnp.where(lane % 64 < 32, high, factor - high)
    for which in range(2):
        for half in range(2):
            lanes = slice(half * 128, (half + 1) * 128)
            for block in range(8):
                rows = slice(block * 8, block * 8 + 8)
                sent_out[which * 16 + half * 8 + block] = jnp.concatenate(
                    [
                        ends[0][which][rows, lanes],
                        ends[1][which][rows, lanes],
                        factor_parts[rows, lanes],
                    ],
                    axis=0,
                ).astype(BF16)
    finish(going)


def convolved(padded, taps, direction, i, columns):
    running = taps[direction, i, 0:1, :] * padded[8 : 8 + ROWS, columns]
    for j in range(1, 4):
        first = 8 + j if direction else 8 - j
        running = running + taps[direction, i, j : j + 1, :] * padded[first : first + ROWS, columns]
    return (running * jax.nn.sigmoid(running)).astype(BF16)


def own_head():
    return (iota((LANES, LANES), 0) // 64 == iota((LANES, LANES), 1) // 64).astype(BF16)


def expand(values, own):
    return jnp.concatenate([values] * 4, axis=0) * own


def seen_by(direction):
    position, other = iota((SPAN, LANES), 0), iota((SPAN, LANES), 1) % SPAN
    return other >= position if direction else other <= position


def meeting_kernel(
    query_in, kv_in, cum_in, shrink_in, start_in, taps,
    queries_out, scores_out, growth_out,
    query, keys, cum, shrink, start, padded, queries, scores, growth, semaphores,
):
    coming = begin(
        [
            (query_in, query),
            (kv_in.at[:, 0], keys),
            (cum_in, cum),
            (shrink_in, shrink),
            (start_in.at[:, :, 0], start),
        ],
        semaphores.at[pl.ds(0, 5)],
    )
    coming[0].wait()
    padded[...] = query[...].astype(F32)
    for direction in range(2):
        queries[direction] = convolved(padded, taps, direction, 0, slice(0, 256))
    going = begin([(queries, queries_out)], semaphores.at[pl.ds(5, 1)])
    finish(coming[1:])
    own = own_head()
    growth[...] = jnp.exp(cum[...])
    going += begin([(growth, growth_out)], semaphores.at[pl.ds(6, 1)])
    for n in range(SPANS):
        rows = slice(n * SPAN, (n + 1) * SPAN)
        for direction in range(2):
            asked = queries[direction, rows, :]
            meeting = nt(asked, expand(keys[direction, rows, :], own))
            meeting = jnp.where(seen_by(direction), meeting, 0.0).astype(BF16)
            scores[direction, rows, :] = growth[direction, rows, :] * (
                nn(meeting, expand(shrink[direction, rows, :], own))
                + nt(asked, expand(start[direction, n], own))
            )
    going += begin([(scores, scores_out)], semaphores.at[pl.ds(7, 1)])
    finish(going)


def scan_kernel(pieces, states_out, wide):
    count = pieces.shape[0]
    first = iota((8, 128), 1) % 64 < 32
    factors, forward, backward = [], [], []
    for i in range(count):
        piece = pieces[i].astype(F32)
        both = piece[16:24]
        factors.append(both + jnp.where(first, pltpu.roll(both, 96, 1), pltpu.roll(both, 32, 1)))
        forward.append(piece[0:8])
        backward.append(piece[8:16])
    state = jnp.zeros((8, 128), F32)
    for i in range(count):
        wide[i, 0:8, :] = state
        state = factors[i] * state + forward[i]
    state = jnp.zeros((8, 128), F32)
    for i in reversed(range(count)):
        wide[i, 8:16, :] = state
        state = factors[i] * state + backward[i]
    states_out[...] = wide[...].astype(BF16)


def head_max(values):
    first = in_first_head(values.shape[0])
    halves = []
    for half in range(2):
        part = values[:, half * 128 : (half + 1) * 128]
        left = jnp.max(jnp.where(first, part, -jnp.inf), axis=1, keepdims=True)
        right = jnp.max(jnp.where(first, -jnp.inf, part), axis=1, keepdims=True)
        halves.append(jnp.where(first, left, right))
    return jnp.concatenate(halves, axis=1)


def attention_kernel(
    own_half,
    queries_in, kv_in, shrink_in, start_in, reach_in, scores_in, growth_in, arrived, gain,
    out,
    queries, values, shrink, start, reach, scores, growth, weighted, mixing, result, entering,
    semaphores,
):
    core = lax.axis_index("core")
    half_index = core if own_half else 1 - core
    rows = pl.ds(pl.multiple_of(half_index * 128, 128), 128)
    spans = pl.ds(half_index * 2, 2)
    coming = begin(
        [
            (reach_in.at[:, spans], reach),
            (queries_in.at[:, rows, :], queries),
            (growth_in.at[:, rows, :], growth),
            (scores_in.at[:, rows, :], scores),
            (shrink_in.at[:, rows, :], shrink),
            (start_in.at[:, spans, 1], start),
            (kv_in.at[:, 1, rows, :], values),
        ],
        semaphores,
    )
    for m in range(32):
        which, half, block = m // 16, (m // 8) % 2, m % 8
        piece = arrived[m].astype(F32)
        for direction in range(2):
            entering[direction, which, block * 8 : block * 8 + 8, half * 128 : half * 128 + 128] = (
                piece[direction * 8 : direction * 8 + 8]
            )
    own = own_head()
    gains = in_lanes(gain[...])
    units = [(direction, n) for direction in range(2) for n in range(2)]
    finish(coming[:4])
    for direction, n in units:
        span = slice(n * SPAN, (n + 1) * SPAN)
        key_state = expand((reach[direction, n] * entering[direction, 0]).astype(BF16), own)
        scores[direction, span, :] = scores[direction, span, :] + growth[
            direction, span, :
        ] * nt(queries[direction, span, :], key_state)
    for direction in range(2):
        total = scores[direction]
        powers = jnp.exp(total - head_max(total))
        attend = powers / nn(powers.astype(BF16), own)
        weighted[direction] = (attend * growth[direction]).astype(BF16)
    finish(coming[4:])
    for direction, n in units:
        span = slice(n * SPAN, (n + 1) * SPAN)
        lessen = expand(shrink[direction, span, :], own)
        mixed = jnp.where(seen_by(direction), nt(weighted[direction, span, :], lessen), 0.0)
        mixing[direction, span, :] = mixed.astype(BF16)
    for direction, n in units:
        span = slice(n * SPAN, (n + 1) * SPAN)
        state = start[direction, n].astype(F32) + reach[direction, n] * entering[direction, 1]
        result[direction, span, :] = nn(
            mixing[direction, span, :], expand(values[direction, span, :], own)
        ) + nn(weighted[direction, span, :], expand(state.astype(BF16), own))
    combined = jnp.zeros((128, LANES), F32)
    for direction in range(2):
        found = result[direction]
        mean = nn((found * found).astype(BF16), own) * (1.0 / 64.0)
        combined = combined + found * lax.rsqrt(mean + EPSILON) * gains
    out[...] = combined.astype(BF16)


def tail_kernel(
    part0, part1, part2, part3, weights, tokens, gain, up, down,
    base_out, out1, out2, out3, residual, update,
):
    head = lax.axis_index("head")
    parts = (part0, part1, part2, part3)
    square = jnp.zeros((ROWS, 1), F32)
    for j in range(4):
        columns = slice(j * 256, (j + 1) * 256)
        total = nn(parts[0][...], weights[0, :, columns])
        for k in range(1, 4):
            total = total + nn(parts[k][...], weights[k, :, columns])
        value = (tokens[j].astype(F32) + total).astype(BF16).astype(F32)
        residual[j] = value
        square = square + jnp.sum(value * value, axis=1, keepdims=True)
    scale = lax.rsqrt(square * (1.0 / 1024.0) + EPSILON)
    entering = jnp.concatenate(
        [(residual[j] * scale * gain_of(gain, j)).astype(BF16) for j in range(4)], axis=1
    )
    hidden = jnp.concatenate(
        [
            jax.nn.gelu(nn(entering, up[:, j * 256 : (j + 1) * 256])).astype(BF16)
            for j in range(4)
        ],
        axis=1,
    )
    for j in range(4):
        update[j] = nn(hidden, down[:, j * 256 : (j + 1) * 256])
    base_out[...] = residual[head] + update[head]
    for k, out in ((1, out1), (2, out2), (3, out3)):
        out[...] = update[lax.rem(head + k, 4)].astype(BF16)


def finish_kernel(base, part1, part2, part3, out):
    core = lax.axis_index("core")
    total = base[...]
    for part in (part1, part2, part3):
        total = total + part[...].astype(F32)
    total = total.astype(BF16)
    out[core] = total[0:128]
    out[1 - core] = total[128:256]


def kernel(body, ins, outs, scratch=(), copies=0, flops=0):
    spaces = {"h": pltpu.HBM, "v": pltpu.VMEM}
    places = [pl.BlockSpec(memory_space=spaces[place]) for place in ins]
    shapes = [
        pltpu.HBM(out[0], out[1]) if out[2] == "h" else jax.ShapeDtypeStruct(out[0], out[1])
        for out in outs
    ]
    out_places = [pl.BlockSpec(memory_space=spaces[out[2]]) for out in outs]
    buffers = [pltpu.VMEM(shape, dtype) for shape, dtype in scratch]
    if copies:
        buffers.append(pltpu.SemaphoreType.DMA((copies,)))
    call = pl.pallas_call(
        body,
        in_specs=places,
        out_specs=out_places,
        out_shape=shapes,
        scratch_shapes=buffers,
        compiler_params=pltpu.CompilerParams(vmem_limit_bytes=32 * 1024 * 1024),
        cost_estimate=pl.CostEstimate(flops=flops, bytes_accessed=1 << 20, transcendentals=0),
    )

    def placed(*arrays):
        return call(
            *[
                pltpu.with_memory_space_constraint(array, pltpu.HBM) if place == "h" else array
                for array, place in zip(arrays, ins)
            ]
        )

    return placed


def shifted(value, k):
    count = lax.axis_size("head")
    return lax.ppermute(value, "head", [(j, (j + k) % count) for j in range(count)])


def local(
    tokens,
    input_norm_gain,
    query_key_value_weight,
    forget_gate_weight,
    convolution_filter_taps,
    slot_forget_rate,
    extra_forget_log,
    head_norm_gain,
    output_projection_weight,
    feedforward_norm_gain,
    up_projection_weight,
    down_projection_weight,
):
    chips = lax.axis_size(CHIPS)
    swap_pairs = [(0, 1), (1, 0)]
    edges, swap, mine = kernel(
        edge_kernel,
        "hh",
        [((2, 8, 256), BF16, "v"), ((136, 256), BF16, "v"), ((128, 256), BF16, "v")],
        [((2, 128, 256), BF16), ((2, 128), F32)],
        copies=2,
    )(tokens, extra_forget_log)
    ahead = [(2 * i - 1, 2 * i) for i in range(1, chips)]
    behind = [(2 * i + 2, 2 * i + 1) for i in range(chips - 1)]
    edges = lax.ppermute(edges, SEQ, ahead + behind)
    other = lax.ppermute(swap, "core", swap_pairs)
    rows = jnp.concatenate([mine, other[:128]], axis=0)
    pick = kernel(pick_kernel, "v", [((8, 256), BF16, "v"), ((8, 256), BF16, "v")])
    sent_edge, kept_edge = pick(edges)
    other_edge = lax.ppermute(sent_edge, "core", swap_pairs)
    halo = jnp.concatenate([kept_edge, other_edge], axis=0)
    halos = [halo]
    for k in (1, 2, 3):
        halos.append(shifted(halo, k))
    qkv_weight = jnp.transpose(query_key_value_weight, (1, 0, 2))
    rows, qkv_weight, gate_weight, out_weight = lax.optimization_barrier(
        (rows, qkv_weight, forget_gate_weight, output_projection_weight)
    )
    parts = [rows]
    for k in (1, 2, 3):
        parts.append(shifted(rows, k))
    qkv_weight, gate_weight, half_weight = kernel(
        warm_kernel,
        "hhh",
        [
            ((3, 1024, 256), BF16, "v"),
            ((1024, 256), BF16, "v"),
            ((128, 1024), BF16, "v"),
        ],
        copies=3,
        flops=10**9,
    )(qkv_weight, gate_weight, out_weight)
    taps = jnp.transpose(convolution_filter_taps, (0, 2, 1, 3))
    halves = (2, ROWS, LANES)
    starts = (2, SPANS, 2, SPAN, LANES)
    reaches = (2, SPANS, SPAN, LANES)
    pieces, query, kv, cum, shrink, start, reach, kept, passed = kernel(
        front_kernel,
        "v" * 15,
        [
            ((32, 24, 128), BF16, "v"),
            ((ROWS + 16, 256), BF16, "h"),
            ((2, 2, ROWS, LANES), BF16, "h"),
            (halves, F32, "h"),
            (halves, BF16, "h"),
            (starts, BF16, "h"),
            (reaches, F32, "h"),
            ((4, 128, 256), BF16, "h"),
            ((4, 128, 256), BF16, "h"),
        ],
        [
            ((ROWS + 16, 768), F32),
            ((ROWS, LANES), F32),
            ((ROWS + 16, 256), BF16),
            ((2, 2, ROWS, LANES), BF16),
            (halves, F32),
            (halves, BF16),
            (starts, BF16),
            (reaches, F32),
            ((4, 128, 256), BF16),
            ((4, 128, 256), BF16),
        ],
        copies=8,
        flops=10**9,
    )(
        *parts,
        *halos,
        input_norm_gain.reshape(8, 128),
        qkv_weight,
        gate_weight,
        taps,
        slot_forget_rate,
        extra_forget_log,
        other[128:136],
    )
    pieces, half_weight, passed = lax.optimization_barrier((pieces, half_weight, passed))
    held = lax.all_to_all(pieces, CHIPS, split_axis=0, concat_axis=0, tiled=True)
    own_weights, other_weights = [], []
    for k in (1, 2, 3):
        own_weights.append(shifted(half_weight, k))
        other_weights.append(lax.ppermute(own_weights[-1], "core", swap_pairs))
    passed = lax.ppermute(passed, "core", swap_pairs)
    meeting = kernel(
        meeting_kernel,
        "hhhhhv",
        [(halves, BF16, "h"), (halves, F32, "h"), (halves, F32, "h")],
        [
            ((ROWS + 16, 256), BF16),
            (halves, BF16),
            (halves, F32),
            (halves, BF16),
            (reaches, BF16),
            ((ROWS + 16, 256), F32),
            (halves, BF16),
            (halves, F32),
            (halves, F32),
        ],
        copies=8,
        flops=10**9,
    )
    queries, scores, growth = meeting(query, kv, cum, shrink, start, taps)
    (prefixes,) = kernel(
        scan_kernel, "v", [((chips, 16, 128), BF16, "v")], [((chips, 16, 128), F32)]
    )(held)
    arrived = lax.all_to_all(prefixes, CHIPS, split_axis=0, concat_axis=0, tiled=True)
    half = (2, 128, LANES)
    reached = (2, 2, SPAN, LANES)
    attention = []
    for own_half in (False, True):
        attend = kernel(
            functools.partial(attention_kernel, own_half),
            "hhhhhhhvv",
            [((128, LANES), BF16, "v")],
            [
                (half, BF16),
                (half, BF16),
                (half, BF16),
                (reached, BF16),
                (reached, F32),
                (half, F32),
                (half, F32),
                (half, BF16),
                (half, BF16),
                (half, F32),
                ((2, 2, SPAN, LANES), F32),
            ],
            copies=7,
            flops=10**9,
        )
        attention += attend(
            queries, kv, shrink, start, reach, scores, growth, arrived, head_norm_gain
        )
    swapped = lax.ppermute(attention[0], "core", swap_pairs)
    attention = jnp.concatenate([attention[1], swapped], axis=0)
    attention, down_weight = lax.optimization_barrier((attention, down_projection_weight))
    attended = [attention]
    for k in (1, 2, 3):
        attended.append(shifted(attention, k))
    warm_tail = kernel(
        warm_tail_kernel,
        "h" * 10,
        [
            ((4, 256, 1024), BF16, "v"),
            ((4, ROWS, 256), BF16, "v"),
            ((1024, 1024), BF16, "v"),
        ],
        copies=10,
        flops=10**9,
    )
    weights, whole_tokens, down_weight = warm_tail(
        output_projection_weight, *own_weights, *other_weights, kept, passed, down_weight
    )
    base, out1, out2, out3 = kernel(
        tail_kernel,
        "v" * 9,
        [((ROWS, 256), F32, "v")] + [((ROWS, 256), BF16, "v")] * 3,
        [((4, ROWS, 256), F32), ((4, ROWS, 256), F32)],
        flops=2 * 10**9,
    )(
        *attended,
        weights,
        whole_tokens,
        feedforward_norm_gain.reshape(8, 128),
        up_projection_weight,
        down_weight,
    )
    sums = [base]
    for k, part in ((1, out1), (2, out2), (3, out3)):
        sums.append(shifted(part, k))
    (out,) = kernel(finish_kernel, "vvvv", [((2, 128, 256), BF16, "v")])(*sums)
    return out


def solution(mesh):
    split = Mesh(
        mesh.devices.reshape(4, 8, 2, mesh.shape["head"]), ("x", "z", "core", "head")
    )
    placed = (
        P(None, SEQ, "head"),
        P(),
        P(None, None, "head"),
        P(None, "head"),
        P(None, None, None, "head"),
        P("head", None),
        P(None, SEQ),
        P("head", None),
        P("head", None),
        P(),
        P(None, "head"),
        P("head", None),
    )

    return jax.shard_map(
        local, mesh=split, in_specs=placed, out_specs=P(None, SEQ, "head"), check_vma=False
    )
```

```python
import jax
import jax.numpy as jnp
from jax import lax
from jax.experimental import pallas as pl
from jax.experimental.pallas import tpu as pltpu
from jax.sharding import Mesh
from jax.sharding import PartitionSpec as P


CHIPS = ("x", "z")
SEQ = ("x", "z", "core")
EPSILON = 1e-06
BF16 = jnp.bfloat16
F32 = jnp.float32
SPAN = 64
ROWS = 256
LANES = 256
SPANS = ROWS // SPAN


def nn(a, b, precision=None):
    return lax.dot_general(
        a, b, (((1,), (0,)), ((), ())), preferred_element_type=F32, precision=precision
    )


def nt(a, b):
    return lax.dot_general(a, b, (((1,), (1,)), ((), ())), preferred_element_type=F32)


def tn(a, b, precision=None):
    return lax.dot_general(
        a, b, (((0,), (0,)), ((), ())), preferred_element_type=F32, precision=precision
    )


def iota(shape, dim):
    return lax.broadcasted_iota(jnp.int32, shape, dim)


def in_first_head(rows):
    return iota((rows, 128), 1) < 64


def compact(blocks):
    first = in_first_head(64)
    left = jnp.where(first, blocks[0:64, 0:128], blocks[64:128, 0:128])
    right = jnp.where(first, blocks[128:192, 128:256], blocks[192:256, 128:256])
    return jnp.concatenate([left, right], axis=1)


def compact_rows(column):
    first = in_first_head(64)
    left = jnp.where(first, column[0:64], column[64:128])
    right = jnp.where(first, column[128:192], column[192:256])
    return jnp.concatenate([left, right], axis=1)


def minus_expm1(x):
    series = 1.0 + x * (1.0 / 7.0)
    for k in (6, 5, 4, 3, 2):
        series = 1.0 + x * (1.0 / k) * series
    return jnp.where(x > -0.3, -x * series, 1.0 - jnp.exp(x))


def exact(matmul, values, zeros_and_ones):
    high = values.astype(BF16)
    rest = values - high.astype(F32)
    middle = rest.astype(BF16)
    low = (rest - middle.astype(F32)).astype(BF16)
    return (
        matmul(low, zeros_and_ones) + matmul(middle, zeros_and_ones)
    ) + matmul(high, zeros_and_ones)


def as_column(row):
    picked = jnp.where(iota((128, 128), 0) == iota((128, 128), 1), row, 0.0)
    return jnp.sum(picked, axis=1, keepdims=True)


def begin(pairs, semaphores):
    copies = [
        pltpu.make_async_copy(source, target, semaphores.at[k])
        for k, (source, target) in enumerate(pairs)
    ]
    for copy in copies:
        copy.start()
    return copies


def finish(copies):
    for copy in copies:
        copy.wait()


def in_lanes(heads):
    return jnp.concatenate([heads[h : h + 1, :] for h in range(4)], axis=1)


def gain_of(gain, source):
    return jnp.concatenate(
        [gain[pl.ds(2 * source, 1), :], gain[pl.ds(2 * source + 1, 1), :]], axis=1
    )


def warm_kernel(qkv_weight, gate_weight, out_weight, qkv_out, gate_out, half_out, semaphores):
    rows = pl.ds(pl.multiple_of(lax.axis_index("core") * 128, 128), 128)
    finish(
        begin(
            [
                (qkv_weight, qkv_out),
                (gate_weight, gate_out),
                (out_weight.at[rows, :], half_out),
            ],
            semaphores,
        )
    )


def warm_tail_kernel(
    weight0, mine1, mine2, mine3, theirs1, theirs2, theirs3, kept, passed, down,
    weights_out, tokens_out, down_out, semaphores,
):
    core = lax.axis_index("core")
    own = pl.ds(pl.multiple_of(core * 128, 128), 128)
    other = pl.ds(pl.multiple_of((1 - core) * 128, 128), 128)
    pairs = [(weight0, weights_out.at[0])]
    for k, mine, theirs in ((1, mine1, theirs1), (2, mine2, theirs2), (3, mine3, theirs3)):
        pairs += [(mine, weights_out.at[k, own]), (theirs, weights_out.at[k, other])]
    pairs += [(kept, tokens_out.at[:, 0:128]), (passed, tokens_out.at[:, 128:256])]
    finish(begin(pairs + [(down, down_out)], semaphores))


def edge_kernel(tokens_in, extra_in, edge_out, swap_out, mine_out, tokens, extra, semaphores):
    core = lax.axis_index("core")
    finish(begin([(tokens_in, tokens), (extra_in, extra)], semaphores))
    mine_out[...] = tokens[core]
    for which in range(2):
        wide = tokens[which].astype(F32)
        edge_out[which] = jnp.where(core == 1, wide[120:128], wide[0:8]).astype(BF16)
    row = extra[pl.ds(1 - core, 1), :]
    high = row.astype(BF16).astype(F32)
    middle = (row - high).astype(BF16).astype(F32)
    low = row - high - middle
    line = iota((8, 256), 0)
    first = jnp.concatenate([high, middle], axis=1)
    second = jnp.concatenate([low, low], axis=1)
    packed = jnp.where(line == 0, first, jnp.where(line == 1, second, 0.0))
    swap_out[0:128] = tokens[1 - core]
    swap_out[128:136] = packed.astype(BF16)


def swap_kernel(local_part, edges, swap_out, kept_out):
    core = lax.axis_index("core")
    swap_out[0:136] = local_part[...]
    swap_out[136:144] = edges[1 - core]
    kept_out[...] = edges[core]


def front_kernel(
    part0, part1, part2, part3, gain, qkv_weight, gate_weight, taps, rate, extra, extra_other,
    sent_out, query_out, kv_out, cum_out, shrink_out, start_out, reach_out, kept_out, passed_out,
    padded, decay, query, kv, cum, shrink, start, reach, kept, passed_on, semaphores,
):
    core = lax.axis_index("core")
    head = lax.axis_index("head")
    parts = (part0, part1, part2, part3)
    sources = [lax.rem(head + 4 - k, 4) for k in range(4)]
    own_rows = pl.multiple_of(core * 128, 128)
    other_rows = pl.multiple_of((1 - core) * 128, 128)
    square = jnp.zeros((ROWS + 16, 1), F32)
    for k in range(4):
        values = parts[k][...]
        kept[sources[k]] = values[0:128]
        passed_on[sources[k]] = values[128:256]
        wide = values.astype(F32)
        square = square + jnp.sum(wide * wide, axis=1, keepdims=True)
    going = begin([(kept, kept_out), (passed_on, passed_out)], semaphores.at[pl.ds(0, 2)])
    scale = lax.rsqrt(square * (1.0 / 1024.0) + EPSILON)
    normed = [
        (parts[k][...].astype(F32) * scale * gain_of(gain, sources[k])).astype(BF16)
        for k in range(4)
    ]
    starts = [pl.multiple_of(source * 256, 256) for source in sources]
    own_pad = pl.multiple_of(8 + core * 128, 8)
    other_pad = pl.multiple_of(8 + (1 - core) * 128, 8)
    a_pad = pl.multiple_of(core * 264, 8)
    b_pad = pl.multiple_of((1 - core) * 264, 8)
    for i in range(3):
        total = nn(normed[0], qkv_weight[i, pl.ds(starts[0], 256), :])
        for k in range(1, 4):
            total = total + nn(normed[k], qkv_weight[i, pl.ds(starts[k], 256), :])
        total = total.astype(BF16).astype(F32)
        columns = slice(i * 256, (i + 1) * 256)
        padded[pl.ds(own_pad, 128), columns] = total[0:128]
        padded[pl.ds(other_pad, 128), columns] = total[128:256]
        padded[pl.ds(a_pad, 8), columns] = total[256:264]
        padded[pl.ds(b_pad, 8), columns] = total[264:272]
    query[...] = padded[:, 0:256].astype(BF16)
    going += begin([(query, query_out)], semaphores.at[pl.ds(2, 1)])
    gate = nn(normed[0], gate_weight[pl.ds(starts[0], 256), :])
    for k in range(1, 4):
        gate = gate + nn(normed[k], gate_weight[pl.ds(starts[k], 256), :])
    own_extra = as_column(extra[pl.ds(core, 1), :])
    sent = extra_other[...].astype(F32)
    other_extra = as_column(sent[0:1, 0:128] + sent[0:1, 128:256] + sent[1:2, 0:128])
    decays = -2.0 * in_lanes(rate[...]) * jax.nn.sigmoid(gate[0:256])
    decay[pl.ds(own_rows, 128), :] = decays[0:128] - own_extra
    decay[pl.ds(other_rows, 128), :] = decays[128:256] - other_extra

    for i in (1, 2):
        columns = slice(i * 256, (i + 1) * 256)
        for direction in range(2):
            kv[direction, i - 1] = convolved(padded, taps, direction, i, columns)
    going += begin([(kv, kv_out)], semaphores.at[pl.ds(3, 1)])

    log_decay = decay[...]
    inflow = minus_expm1(log_decay)
    row, col = iota((ROWS, ROWS), 0), iota((ROWS, ROWS), 1)
    same = (row // SPAN) == (col // SPAN)
    earlier = (same & (col <= row)).astype(BF16)
    later = (same & (col >= row)).astype(BF16)
    spans = (iota((ROWS, 128 * SPANS), 0) // SPAN == iota((ROWS, 128 * SPANS), 1) // 128).astype(BF16)
    for direction in range(2):
        order = later if direction else earlier
        cum[direction] = exact(lambda part, ones: nn(ones, part), log_decay, order)
        shrink[direction] = (jnp.exp(-cum[direction]) * inflow).astype(BF16)
    going += begin([(cum, cum_out), (shrink, shrink_out)], semaphores.at[pl.ds(4, 2)])
    span_totals = exact(tn, log_decay, spans)
    totals = [compact_rows(span_totals[:, n * 128 : (n + 1) * 128]) for n in range(SPANS)]
    factors = [jnp.exp(total) for total in totals]
    units = [(direction, n) for direction in range(2) for n in range(SPANS)]
    added = {}
    for direction, n in units:
        rows = slice(n * SPAN, (n + 1) * SPAN)
        local = cum[direction, rows, :]
        last = local[0:1] if direction else local[SPAN - 1 : SPAN]
        remain = (jnp.exp(last - local) * inflow[rows]).astype(BF16)
        for which in range(2):
            added[direction, n, which] = compact(tn(remain, kv[direction, which, rows, :]))
    ends = []
    for direction in range(2):
        states = [jnp.zeros((SPAN, LANES), F32), jnp.zeros((SPAN, LANES), F32)]
        passed = jnp.zeros((SPAN, LANES), F32)
        for n in reversed(range(SPANS)) if direction else range(SPANS):
            reach[direction, n] = jnp.exp(passed)
            for which in range(2):
                start[direction, n, which] = states[which].astype(BF16)
                states[which] = factors[n] * states[which] + added[direction, n, which]
            passed = passed + totals[n]
        ends.append(states)
    going += begin([(start, start_out), (reach, reach_out)], semaphores.at[pl.ds(6, 2)])
    factor = jnp.exp(totals[0] + totals[1] + totals[2] + totals[3])
    high = factor.astype(BF16).astype(F32)
    lane = iota((SPAN, LANES), 1)
    factor_parts = jnp.where(lane % 64 < 32, high, factor - high)
    for which in range(2):
        for half in range(2):
            lanes = slice(half * 128, (half + 1) * 128)
            for block in range(8):
                rows = slice(block * 8, block * 8 + 8)
                sent_out[which * 16 + half * 8 + block] = jnp.concatenate(
                    [
                        ends[0][which][rows, lanes],
                        ends[1][which][rows, lanes],
                        factor_parts[rows, lanes],
                    ],
                    axis=0,
                ).astype(BF16)
    finish(going)


def convolved(padded, taps, direction, i, columns):
    running = taps[direction, i, 0:1, :] * padded[8 : 8 + ROWS, columns]
    for j in range(1, 4):
        first = 8 + j if direction else 8 - j
        running = running + taps[direction, i, j : j + 1, :] * padded[first : first + ROWS, columns]
    return (running * jax.nn.sigmoid(running)).astype(BF16)


def own_head():
    return (iota((LANES, LANES), 0) // 64 == iota((LANES, LANES), 1) // 64).astype(BF16)


def expand(values, own):
    return jnp.concatenate([values] * 4, axis=0) * own


def seen_by(direction):
    position, other = iota((SPAN, LANES), 0), iota((SPAN, LANES), 1) % SPAN
    return other >= position if direction else other <= position


def meeting_kernel(
    query_in, kv_in, cum_in, shrink_in, start_in, taps,
    queries_out, scores_out, growth_out,
    query, keys, cum, shrink, start, padded, queries, scores, growth, semaphores,
):
    coming = begin(
        [
            (query_in, query),
            (kv_in.at[:, 0], keys),
            (cum_in, cum),
            (shrink_in, shrink),
            (start_in.at[:, :, 0], start),
        ],
        semaphores.at[pl.ds(0, 5)],
    )
    coming[0].wait()
    padded[...] = query[...].astype(F32)
    for direction in range(2):
        queries[direction] = convolved(padded, taps, direction, 0, slice(0, 256))
    going = begin([(queries, queries_out)], semaphores.at[pl.ds(5, 1)])
    finish(coming[1:])
    own = own_head()
    growth[...] = jnp.exp(cum[...])
    going += begin([(growth, growth_out)], semaphores.at[pl.ds(6, 1)])
    for n in range(SPANS):
        rows = slice(n * SPAN, (n + 1) * SPAN)
        for direction in range(2):
            asked = queries[direction, rows, :]
            meeting = nt(asked, expand(keys[direction, rows, :], own))
            meeting = jnp.where(seen_by(direction), meeting, 0.0).astype(BF16)
            scores[direction, rows, :] = growth[direction, rows, :] * (
                nn(meeting, expand(shrink[direction, rows, :], own))
                + nt(asked, expand(start[direction, n], own))
            )
    going += begin([(scores, scores_out)], semaphores.at[pl.ds(7, 1)])
    finish(going)


def scan_kernel(pieces, states_out, wide):
    count = pieces.shape[0]
    first = iota((8, 128), 1) % 64 < 32
    factors, forward, backward = [], [], []
    for i in range(count):
        piece = pieces[i].astype(F32)
        both = piece[16:24]
        factors.append(both + jnp.where(first, pltpu.roll(both, 96, 1), pltpu.roll(both, 32, 1)))
        forward.append(piece[0:8])
        backward.append(piece[8:16])
    state = jnp.zeros((8, 128), F32)
    for i in range(count):
        wide[i, 0:8, :] = state
        state = factors[i] * state + forward[i]
    state = jnp.zeros((8, 128), F32)
    for i in reversed(range(count)):
        wide[i, 8:16, :] = state
        state = factors[i] * state + backward[i]
    states_out[...] = wide[...].astype(BF16)


def head_max(values):
    first = in_first_head(values.shape[0])
    halves = []
    for half in range(2):
        part = values[:, half * 128 : (half + 1) * 128]
        left = jnp.max(jnp.where(first, part, -jnp.inf), axis=1, keepdims=True)
        right = jnp.max(jnp.where(first, -jnp.inf, part), axis=1, keepdims=True)
        halves.append(jnp.where(first, left, right))
    return jnp.concatenate(halves, axis=1)


def attend_other_kernel(
    reach_in, queries_in, growth_in, scores_in, shrink_in, start_in, kv_in, arrived, gain,
    out, entering,
    next_reach, next_queries, next_growth, next_scores, next_shrink, next_start, next_values,
    reach, queries, growth, scores, shrink, start, values, weighted, mixing, result, semaphores,
):
    core = lax.axis_index("core")

    def copies(half_index, targets, first):
        rows = pl.ds(pl.multiple_of(half_index * 128, 128), 128)
        spans = pl.ds(half_index * 2, 2)
        sources = (
            reach_in.at[:, spans],
            queries_in.at[:, rows, :],
            growth_in.at[:, rows, :],
            scores_in.at[:, rows, :],
            shrink_in.at[:, rows, :],
            start_in.at[:, spans, 1],
            kv_in.at[:, 1, rows, :],
        )
        return begin(list(zip(sources, targets)), semaphores.at[pl.ds(first, 7)])

    coming = copies(1 - core, (reach, queries, growth, scores, shrink, start, values), 0)
    later = copies(
        core,
        (next_reach, next_queries, next_growth, next_scores, next_shrink, next_start, next_values),
        7,
    )
    for m in range(32):
        which, half, block = m // 16, (m // 8) % 2, m % 8
        piece = arrived[m].astype(F32)
        for direction in range(2):
            entering[direction, which, block * 8 : block * 8 + 8, half * 128 : half * 128 + 128] = (
                piece[direction * 8 : direction * 8 + 8]
            )
    finish(coming)
    attend(
        reach, queries, growth, scores, shrink, start, values, entering, gain,
        out, scores, weighted, mixing, result,
    )
    finish(later)


def attend(
    reach, queries, growth, scores, shrink, start, values, entering, gain,
    out, totals, weighted, mixing, result,
):
    own = own_head()
    gains = in_lanes(gain[...])
    units = [(direction, n) for direction in range(2) for n in range(2)]
    for direction, n in units:
        span = slice(n * SPAN, (n + 1) * SPAN)
        key_state = expand((reach[direction, n] * entering[direction, 0]).astype(BF16), own)
        totals[direction, span, :] = scores[direction, span, :] + growth[
            direction, span, :
        ] * nt(queries[direction, span, :], key_state)
    for direction in range(2):
        total = totals[direction]
        powers = jnp.exp(total - head_max(total))
        attend = powers / nn(powers.astype(BF16), own)
        weighted[direction] = (attend * growth[direction]).astype(BF16)
    for direction, n in units:
        span = slice(n * SPAN, (n + 1) * SPAN)
        lessen = expand(shrink[direction, span, :], own)
        mixed = jnp.where(seen_by(direction), nt(weighted[direction, span, :], lessen), 0.0)
        mixing[direction, span, :] = mixed.astype(BF16)
    for direction, n in units:
        span = slice(n * SPAN, (n + 1) * SPAN)
        state = start[direction, n].astype(F32) + reach[direction, n] * entering[direction, 1]
        result[direction, span, :] = nn(
            mixing[direction, span, :], expand(values[direction, span, :], own)
        ) + nn(weighted[direction, span, :], expand(state.astype(BF16), own))
    combined = jnp.zeros((128, LANES), F32)
    for direction in range(2):
        found = result[direction]
        mean = nn((found * found).astype(BF16), own) * (1.0 / 64.0)
        combined = combined + found * lax.rsqrt(mean + EPSILON) * gains
    out[...] = combined.astype(BF16)


def tail_kernel(
    part0, part1, part2, part3, weights, tokens, gain, up, down,
    base_out, out1, out2, out3, residual, update,
):
    head = lax.axis_index("head")
    parts = (part0, part1, part2, part3)
    square = jnp.zeros((ROWS, 1), F32)
    for j in range(4):
        columns = slice(j * 256, (j + 1) * 256)
        total = nn(parts[0][...], weights[0, :, columns])
        for k in range(1, 4):
            total = total + nn(parts[k][...], weights[k, :, columns])
        value = (tokens[j].astype(F32) + total).astype(BF16).astype(F32)
        residual[j] = value
        square = square + jnp.sum(value * value, axis=1, keepdims=True)
    scale = lax.rsqrt(square * (1.0 / 1024.0) + EPSILON)
    entering = jnp.concatenate(
        [(residual[j] * scale * gain_of(gain, j)).astype(BF16) for j in range(4)], axis=1
    )
    hidden = jnp.concatenate(
        [
            jax.nn.gelu(nn(entering, up[:, j * 256 : (j + 1) * 256])).astype(BF16)
            for j in range(4)
        ],
        axis=1,
    )
    for j in range(4):
        update[j] = nn(hidden, down[:, j * 256 : (j + 1) * 256])
    base_out[...] = residual[head] + update[head]
    for k, out in ((1, out1), (2, out2), (3, out3)):
        out[...] = update[lax.rem(head + k, 4)].astype(BF16)


def finish_kernel(base, part1, part2, part3, out):
    core = lax.axis_index("core")
    total = base[...]
    for part in (part1, part2, part3):
        total = total + part[...].astype(F32)
    total = total.astype(BF16)
    out[core] = total[0:128]
    out[1 - core] = total[128:256]


def kernel(body, ins, outs, scratch=(), copies=0, flops=0):
    spaces = {"h": pltpu.HBM, "v": pltpu.VMEM}
    places = [pl.BlockSpec(memory_space=spaces[place]) for place in ins]
    shapes = [
        pltpu.HBM(out[0], out[1]) if out[2] == "h" else jax.ShapeDtypeStruct(out[0], out[1])
        for out in outs
    ]
    out_places = [pl.BlockSpec(memory_space=spaces[out[2]]) for out in outs]
    buffers = [pltpu.VMEM(shape, dtype) for shape, dtype in scratch]
    if copies:
        buffers.append(pltpu.SemaphoreType.DMA((copies,)))
    call = pl.pallas_call(
        body,
        in_specs=places,
        out_specs=out_places,
        out_shape=shapes,
        scratch_shapes=buffers,
        compiler_params=pltpu.CompilerParams(vmem_limit_bytes=32 * 1024 * 1024),
        cost_estimate=pl.CostEstimate(flops=flops, bytes_accessed=1 << 20, transcendentals=0),
    )

    def placed(*arrays):
        return call(
            *[
                pltpu.with_memory_space_constraint(array, pltpu.HBM) if place == "h" else array
                for array, place in zip(arrays, ins)
            ]
        )

    return placed


def shifted(value, k):
    count = lax.axis_size("head")
    return lax.ppermute(value, "head", [(j, (j + k) % count) for j in range(count)])


def local(
    tokens,
    input_norm_gain,
    query_key_value_weight,
    forget_gate_weight,
    convolution_filter_taps,
    slot_forget_rate,
    extra_forget_log,
    head_norm_gain,
    output_projection_weight,
    feedforward_norm_gain,
    up_projection_weight,
    down_projection_weight,
):
    chips = lax.axis_size(CHIPS)
    swap_pairs = [(0, 1), (1, 0)]
    edges, swap, mine = kernel(
        edge_kernel,
        "hh",
        [((2, 8, 256), BF16, "v"), ((136, 256), BF16, "v"), ((128, 256), BF16, "v")],
        [((2, 128, 256), BF16), ((2, 128), F32)],
        copies=2,
    )(tokens, extra_forget_log)
    ahead = [(2 * i - 1, 2 * i) for i in range(1, chips)]
    behind = [(2 * i + 2, 2 * i + 1) for i in range(chips - 1)]
    edges = lax.ppermute(edges, SEQ, ahead + behind)
    swap, kept_edge = kernel(
        swap_kernel, "vv", [((144, 256), BF16, "v"), ((8, 256), BF16, "v")]
    )(swap, edges)
    other = lax.ppermute(swap, "core", swap_pairs)
    rows = jnp.concatenate([mine, other[:128], kept_edge, other[136:]], axis=0)
    qkv_weight = jnp.transpose(query_key_value_weight, (1, 0, 2))
    rows, qkv_weight, gate_weight, out_weight = lax.optimization_barrier(
        (rows, qkv_weight, forget_gate_weight, output_projection_weight)
    )
    parts = [rows]
    for k in (1, 2, 3):
        parts.append(shifted(rows, k))
    qkv_weight, gate_weight, half_weight = kernel(
        warm_kernel,
        "hhh",
        [
            ((3, 1024, 256), BF16, "v"),
            ((1024, 256), BF16, "v"),
            ((128, 1024), BF16, "v"),
        ],
        copies=3,
        flops=10**9,
    )(qkv_weight, gate_weight, out_weight)
    taps = jnp.transpose(convolution_filter_taps, (0, 2, 1, 3))
    halves = (2, ROWS, LANES)
    starts = (2, SPANS, 2, SPAN, LANES)
    reaches = (2, SPANS, SPAN, LANES)
    pieces, query, kv, cum, shrink, start, reach, kept, passed = kernel(
        front_kernel,
        "v" * 11,
        [
            ((32, 24, 128), BF16, "v"),
            ((ROWS + 16, 256), BF16, "h"),
            ((2, 2, ROWS, LANES), BF16, "h"),
            (halves, F32, "h"),
            (halves, BF16, "h"),
            (starts, BF16, "h"),
            (reaches, F32, "h"),
            ((4, 128, 256), BF16, "h"),
            ((4, 128, 256), BF16, "h"),
        ],
        [
            ((ROWS + 16, 768), F32),
            ((ROWS, LANES), F32),
            ((ROWS + 16, 256), BF16),
            ((2, 2, ROWS, LANES), BF16),
            (halves, F32),
            (halves, BF16),
            (starts, BF16),
            (reaches, F32),
            ((4, 128, 256), BF16),
            ((4, 128, 256), BF16),
        ],
        copies=8,
        flops=10**9,
    )(
        *parts,
        input_norm_gain.reshape(8, 128),
        qkv_weight,
        gate_weight,
        taps,
        slot_forget_rate,
        extra_forget_log,
        other[128:136],
    )
    pieces, half_weight, passed = lax.optimization_barrier((pieces, half_weight, passed))
    held = lax.all_to_all(pieces, CHIPS, split_axis=0, concat_axis=0, tiled=True)
    own_weights, other_weights = [], []
    for k in (1, 2, 3):
        own_weights.append(shifted(half_weight, k))
        other_weights.append(lax.ppermute(own_weights[-1], "core", swap_pairs))
    passed = lax.ppermute(passed, "core", swap_pairs)
    meeting = kernel(
        meeting_kernel,
        "hhhhhv",
        [(halves, BF16, "h"), (halves, F32, "h"), (halves, F32, "h")],
        [
            ((ROWS + 16, 256), BF16),
            (halves, BF16),
            (halves, F32),
            (halves, BF16),
            (reaches, BF16),
            ((ROWS + 16, 256), F32),
            (halves, BF16),
            (halves, F32),
            (halves, F32),
        ],
        copies=8,
        flops=10**9,
    )
    queries, scores, growth = meeting(query, kv, cum, shrink, start, taps)
    (prefixes,) = kernel(
        scan_kernel, "v", [((chips, 16, 128), BF16, "v")], [((chips, 16, 128), F32)]
    )(held)
    arrived = lax.all_to_all(prefixes, CHIPS, split_axis=0, concat_axis=0, tiled=True)
    half = (2, 128, LANES)
    reached = (2, 2, SPAN, LANES)
    buffers = [
        (reached, F32),
        (half, BF16),
        (half, F32),
        (half, F32),
        (half, BF16),
        (reached, BF16),
        (half, BF16),
    ]
    work = [(half, BF16), (half, BF16), (half, F32)]
    attend_other = kernel(
        attend_other_kernel,
        "hhhhhhhvv",
        [((128, LANES), BF16, "v"), ((2, 2, SPAN, LANES), F32, "v")]
        + [(*buffer, "v") for buffer in buffers],
        buffers + work,
        copies=14,
        flops=10**9,
    )
    attend_own = kernel(
        attend, "v" * 9, [((128, LANES), BF16, "v")], [(half, F32)] + work, flops=10**9
    )
    other_rows, entering, *later = attend_other(
        reach, queries, growth, scores, shrink, start, kv, arrived, head_norm_gain
    )
    (own_rows,) = attend_own(*later, entering, head_norm_gain)
    attention = [other_rows, own_rows]
    swapped = lax.ppermute(attention[0], "core", swap_pairs)
    attention = jnp.concatenate([attention[1], swapped], axis=0)
    attention, down_weight = lax.optimization_barrier((attention, down_projection_weight))
    attended = [attention]
    for k in (1, 2, 3):
        attended.append(shifted(attention, k))
    warm_tail = kernel(
        warm_tail_kernel,
        "h" * 10,
        [
            ((4, 256, 1024), BF16, "v"),
            ((4, ROWS, 256), BF16, "v"),
            ((1024, 1024), BF16, "v"),
        ],
        copies=10,
        flops=10**9,
    )
    weights, whole_tokens, down_weight = warm_tail(
        output_projection_weight, *own_weights, *other_weights, kept, passed, down_weight
    )
    base, out1, out2, out3 = kernel(
        tail_kernel,
        "v" * 9,
        [((ROWS, 256), F32, "v")] + [((ROWS, 256), BF16, "v")] * 3,
        [((4, ROWS, 256), F32), ((4, ROWS, 256), F32)],
        flops=2 * 10**9,
    )(
        *attended,
        weights,
        whole_tokens,
        feedforward_norm_gain.reshape(8, 128),
        up_projection_weight,
        down_weight,
    )
    sums = [base]
    for k, part in ((1, out1), (2, out2), (3, out3)):
        sums.append(shifted(part, k))
    (out,) = kernel(finish_kernel, "vvvv", [((2, 128, 256), BF16, "v")])(*sums)
    return out


def solution(mesh):
    split = Mesh(
        mesh.devices.reshape(4, 8, 2, mesh.shape["head"]), ("x", "z", "core", "head")
    )
    placed = (
        P(None, SEQ, "head"),
        P(),
        P(None, None, "head"),
        P(None, "head"),
        P(None, None, None, "head"),
        P("head", None),
        P(None, SEQ),
        P("head", None),
        P("head", None),
        P(),
        P(None, "head"),
        P("head", None),
    )

    return jax.shard_map(
        local, mesh=split, in_specs=placed, out_specs=P(None, SEQ, "head"), check_vma=False
    )
```
